256 devices in a mesh: slides: 2 (over y), seq: 32 (over z, core), sub: 4 (over x).
Axes of the slice: x: 4, y: 2, z: 16, core: 2. Of those that a mesh axis runs over, the one named last changes fastest.
The devices are a block of a 4x16x16 slice.
Arguments:
- q_heads: bfloat16 [65536, 768], P(('slides', 'seq'), 'sub'), parts along dimension 0, may hold values from -8 to 8
- k_heads: bfloat16 [65536, 768], P(('slides', 'seq'), 'sub'), parts along dimension 0, may hold values from -8 to 8
- v_heads: bfloat16 [65536, 768], P(('slides', 'seq'), 'sub'), parts along dimension 0, may hold values from -6 to 6
- w_out: bfloat16 [768, 768], replicated, may hold values from -0.21875 to 0.21875
- offsets: int32 [2, 16], replicated, may hold values from 0 to 15, as said below
- valid: int32 [2], P('slides'), parts along dimension 0, may hold values from 31745 to 32768
Outputs:
- mixed: bfloat16 [65536, 768], P(('slides', 'seq'), 'sub'), parts along dimension 0
The draws below stay inside these ranges and needn't reach their ends.
There are 2 independent parts, one for each index of `slides`. The reference program is written for one: setup_inputs(seed, part) draws one part's arguments, and reference() takes and returns one part's arrays. A program takes and returns all parts, laid end to end along the dimension named above; an argument that names none is the same for every part. Nothing has to cross between parts.
Inputs may be any that keep to these rules, and one draw needn't show every extreme that they name: `offsets`: row 0 lies below 4, row 1 below 16. Tiles at positions valid[0] and beyond are padding.
All inputs are finite; a program needn't handle non-finite values.
Results may differ from the reference program's by a relative error of at most 0.012.
Values may be sent and summed in bfloat16 or wider, within the bound.
No kernel may reach another device: no remote copies, remote signals or barrier semaphores. Data moves between devices by JAX's collectives and lax.ppermute only.
A program may use at most 64 MiB of HBM per device.

```python
import jax
import jax.numpy as jnp
from jax import lax

D = 768
H = 16
HS = 48
TOK_DEV = 1024
GROUP = 4
R1 = 4
R2 = 16
TOKENS = 32768


def paired_fields(key):
    first_key = jax.random.fold_in(key, 101)
    second_key = jax.random.fold_in(key, 202)
    query = jnp.clip(2.0 * jax.random.normal(first_key, (TOKENS, D), jnp.float32), -8.0, 8.0)
    key_out = jnp.clip(2.0 * jax.random.normal(second_key, (TOKENS, D), jnp.float32), -8.0, 8.0)
    return (query, key_out)


def draw_q_heads(key, part):
    return paired_fields(key)[0].astype(jnp.bfloat16)


def draw_k_heads(key, part):
    return paired_fields(key)[1].astype(jnp.bfloat16)


def draw_offsets(key, part):
    middle = jax.random.randint(jax.random.fold_in(key, 7), (H,), 0, R1).astype(jnp.int32)
    widest = jax.random.randint(jax.random.fold_in(key, 8), (H,), 0, R2).astype(jnp.int32)
    low_head = jax.random.randint(jax.random.fold_in(key, 9), (), 0, H)
    high_head = jax.random.randint(jax.random.fold_in(key, 10), (), 0, H)
    top_head = jax.random.randint(jax.random.fold_in(key, 11), (), 0, H)
    middle = middle.at[low_head].set(0)
    middle = middle.at[(low_head + 1 + top_head % (H - 1)) % H].set(R1 - 1)
    widest = widest.at[high_head].set(R2 - 1)
    return jnp.stack([middle, widest], axis=0).astype(jnp.int32)


def shard_levels(own_key, extent, shards, least, top_value):
    level, own = 1.0, jax.random.fold_in(own_key, 6)
    for axis_at, shards_of in shards:
        steps = jnp.exp(jax.random.uniform(jax.random.fold_in(own, axis_at), (shards_of,), jnp.float32, least / len(shards), top_value / len(shards)))
        level = level * jnp.repeat(steps, extent[axis_at] // shards_of).reshape([-1 if axis == axis_at else 1 for axis in range(len(extent))])
    return level


def noise(key, dims, width, most, cuts=(), kind=jnp.bfloat16):
    values = width * jax.random.normal(key, dims, jnp.float32)
    if cuts:
        values = values * shard_levels(key, dims, cuts, -0.22, 0.18)
    return jnp.clip(values, -most, most).astype(kind)


def setup_inputs(seed: int = 0, part: int = 0) -> dict:
    keys = jax.random.split(jax.random.key(seed), 7)
    own_keys = jax.random.split(jax.random.fold_in(keys[6], part), 7)
    q_heads = draw_q_heads(jax.random.fold_in(jax.random.fold_in(keys[6], part), 71), part)
    k_heads = draw_k_heads(jax.random.fold_in(jax.random.fold_in(keys[6], part), 71), part)
    v_heads = noise(own_keys[2], (TOKENS, D), 1.0, 6.0, ((0, 32), (1, 4)))
    w_out = noise(keys[3], (D, D), D ** -0.5, 0.21875)
    offsets = draw_offsets(jax.random.fold_in(keys[6], 71), part)
    valid = jax.random.randint(own_keys[5], (1,), TOKENS - TOK_DEV + 1, TOKENS + 1).astype(jnp.int32)
    return dict(q_heads=q_heads, k_heads=k_heads, v_heads=v_heads, w_out=w_out, offsets=offsets, valid=valid)


NEG_FILL = -1.0e30


def pick_rows(source, stride, chosen):
    grouped = source.reshape(source.shape[0] // stride, stride, source.shape[1], source.shape[2])
    onehot = jnp.arange(stride, dtype=jnp.int32)[:, None] == chosen[None, :]
    return jnp.sum(jnp.where(onehot[None, :, :, None], grouped, jnp.zeros((), source.dtype)), axis=1)


def spread_back(maxima, totals, numer, stride, chosen):
    onehot = (jnp.arange(stride, dtype=jnp.int32)[:, None] == chosen[None, :])[None]
    count = maxima.shape[0] * stride
    full_max = jnp.where(onehot, maxima[:, None, :], NEG_FILL).reshape(count, maxima.shape[1])
    full_tot = jnp.where(onehot, totals[:, None, :], 0.0).reshape(count, maxima.shape[1])
    full_num = jnp.where(onehot[..., None], numer[:, None, :, :], 0.0).reshape(count, numer.shape[1], numer.shape[2])
    return full_max, full_tot, full_num


def one_branch(query, key_in, value, seg_len, stride, chosen, limit):
    total_rows = query.shape[0]
    heads = query.shape[1]
    q_sel = pick_rows(query, stride, chosen)
    k_sel = pick_rows(key_in, stride, chosen)
    v_sel = pick_rows(value, stride, chosen)
    per_seg = seg_len // stride
    n_segs = total_rows // seg_len
    positions = jnp.arange(total_rows // stride, dtype=jnp.int32)[:, None] * stride + chosen[None, :]
    live = positions < limit

    def arrange(block):
        moved = jnp.moveaxis(block, 1, 0)
        return moved.reshape((heads * n_segs, per_seg) + moved.shape[2:])

    def attend(items):
        q_blk, k_blk, v_blk, l_blk = items
        scores = jnp.dot(q_blk, k_blk.T, preferred_element_type=jnp.float32) * (HS ** -0.5)
        scores = jnp.where(l_blk[None, :], scores, NEG_FILL)
        peak = jnp.max(scores, axis=1)
        probs = jnp.exp(scores - peak[:, None])
        mass = jnp.sum(probs, axis=1)
        numer = jnp.dot(probs.astype(jnp.bfloat16), v_blk, preferred_element_type=jnp.float32)
        return peak, mass, numer

    peak, mass, numer = lax.map(attend, (arrange(q_sel), arrange(k_sel), arrange(v_sel), arrange(live)))
    peak = peak.reshape(heads, total_rows // stride).T
    mass = mass.reshape(heads, total_rows // stride).T
    numer = jnp.moveaxis(numer.reshape(heads, total_rows // stride, HS), 0, 1)
    return spread_back(peak, mass, numer, stride, chosen)


def reference(q_heads, k_heads, v_heads, w_out, offsets, valid):
    total_rows = q_heads.shape[0]
    query = q_heads.reshape(total_rows, H, HS)
    key_in = k_heads.reshape(total_rows, H, HS)
    value = v_heads.reshape(total_rows, H, HS)
    limit = valid[0]
    zero_offs = jnp.zeros((H,), jnp.int32)
    branches = [
        one_branch(query, key_in, value, TOK_DEV, 1, zero_offs, limit),
        one_branch(query, key_in, value, GROUP * TOK_DEV, R1, offsets[0], limit),
        one_branch(query, key_in, value, TOKENS, R2, offsets[1], limit),
    ]
    top = jnp.maximum(jnp.maximum(branches[0][0], branches[1][0]), branches[2][0])
    denom = jnp.zeros_like(top)
    numer = jnp.zeros_like(branches[0][2])
    for peak, mass, partial_num in branches:
        weight = jnp.exp(peak - top)
        denom = denom + weight * mass
        numer = numer + weight[..., None] * partial_num
    attn = (numer / denom[..., None]).reshape(total_rows, D).astype(jnp.bfloat16)
    projected = jnp.dot(attn, w_out, preferred_element_type=jnp.float32)
    keep = jnp.arange(total_rows, dtype=jnp.int32) < limit
    return jnp.where(keep[:, None], projected, 0.0).astype(jnp.bfloat16)
```

```python
import functools
import math

import jax
import jax.numpy as jnp
from jax import lax
from jax.experimental import pallas as pl
from jax.experimental.pallas import tpu as pltpu
from jax.sharding import PartitionSpec as P

HS = 48
R1 = 4
R2 = 16
LOG2_SCALE = HS ** (-0.5) * math.log2(math.e)
MASKED = -1e6

F32 = jnp.float32
BF16 = jnp.bfloat16


VMEM = pl.BlockSpec(memory_space=pltpu.VMEM)
SMEM = pl.BlockSpec(memory_space=pltpu.SMEM)


def lanes(width=128):
    return lax.broadcasted_iota(jnp.int32, (1, width), 1)


def head_lanes(h):
    lane = lanes(256)
    return ((lane >= h * HS) & (lane < (h + 1) * HS)) | (lane == 4 * HS + h)


def head_tile(h, tile):
    return head_lanes(h)[:, tile * 128 : (tile + 1) * 128]


def head_tile_all(h, tile):
    lane = lanes()
    if tile == 0:
        return (lane >= h * HS) & (lane < (h + 1) * HS)
    low = h * HS - 128
    return ((lane >= low) & (lane < low + HS) & (lane < 64)) | (lane == 64 + h) | (lane == 68 + h)


def attend(q, k, v):
    scores = lax.dot_general(q, k, (((1,), (1,)), ((), ())), preferred_element_type=F32)
    peak = jnp.max(scores, axis=1, keepdims=True) * LOG2_SCALE
    probs = jnp.exp2(scores * LOG2_SCALE - peak)
    return peak, jnp.dot(probs.astype(BF16), v, preferred_element_type=F32)


def prep_kernel(offs, k_ref, v_ref, mid_ref, wide_ref, kf, vf, tf, uf):
    kf[...] = k_ref[:, :128].astype(F32)
    vf[...] = v_ref[:, :128].astype(F32)
    tf[:, :64] = k_ref[:, 128:192].astype(F32)
    uf[:, :64] = v_ref[:, 128:192].astype(F32)
    tf[...] = jnp.where(lanes() < 64, tf[...], pltpu.roll(uf[...], 64, 1))
    lane = lanes()
    for row, stride, out in ((0, R1, mid_ref), (1, R2, wide_ref)):
        count = out.shape[0]

        def pick(ref, h):
            return ref[pl.ds(offs[row, h], count, stride=stride), :]

        for tile, ref in ((0, kf), (1, vf)):
            joined = jnp.where(lane < HS, pick(ref, 0), jnp.where(lane < 2 * HS, pick(ref, 1), pick(ref, 2)))
            out[:, tile * 128 : (tile + 1) * 128] = joined.astype(BF16)
        joined = jnp.where(lane % 64 < 16, pick(tf, 2), pick(tf, 3))
        out[:, 256:384] = joined.astype(BF16)


def near_kernel(scal, offs, q_ref, k_ref, v_ref, acc_ref, qm_ref, qw_ref, qa, ka, va, q0, q1):
    rows = q_ref.shape[0]
    lane = lanes()
    mass = (lane >= 64) & (lane < 68)
    ones = jnp.broadcast_to(jnp.where(mass, 1.0, 0.0), (rows, 128))
    q0[...] = q_ref[:, :128].astype(F32)
    q1[...] = ones
    q1[:, :64] = q_ref[:, 128:192].astype(F32)
    qa[:, :128] = q_ref[:, :128]
    qa[:, 128:256] = q1[...].astype(BF16)
    position = scal[0] + lax.broadcasted_iota(jnp.int32, (rows, 1), 0)
    dead = jnp.where(position < scal[1], 0.0, MASKED)
    ka[:, :128] = k_ref[:, :128]
    ka[:, 128:256] = jnp.where(mass, dead, jnp.zeros((rows, 128), F32)).astype(BF16)
    ka[:, 128:192] = k_ref[:, 128:192]
    va[:, :128] = v_ref[:, :128]
    va[:, 128:256] = ones.astype(BF16)
    va[:, 128:192] = v_ref[:, 128:192]

    for row, stride, out in ((0, R1, qm_ref), (1, R2, qw_ref)):
        count = rows // stride
        for h in range(4):
            for tile, ref in ((0, q0), (1, q1)):
                picked = ref[pl.ds(offs[row, h], count, stride=stride), :]
                picked = jnp.where(head_tile(h, tile), picked, 0.0)
                out[h * count : (h + 1) * count, tile * 128 : (tile + 1) * 128] = picked.astype(BF16)

    chunk = 256

    def step(i, carry):
        at = pl.ds(pl.multiple_of(i * chunk, chunk), chunk)
        q = qa[at, :]
        acc = jnp.zeros((chunk, 256), F32)
        for h in range(4):
            qh = jnp.where(head_lanes(h), q, jnp.zeros((), BF16))
            peak, out = attend(qh, ka[...], va[...])
            acc = jnp.where(head_lanes(h), out, acc)
            acc = jnp.where(lanes(256) == 4 * HS + 4 + h, peak, acc)
        acc_ref[0, at, :] = acc[:, :128]
        acc_ref[1, at, :] = acc[:, 128:]
        return carry

    lax.fori_loop(0, rows // chunk, step, 0)


def open_piece(piece, first, stride, offs, row, valid, ka, va, at):
    count = piece.shape[0]
    lane = lanes()
    shift = jnp.zeros((1, 128), jnp.int32)
    for h in range(4):
        shift = jnp.where(lane == 64 + h, offs[row, h], shift)
    position = first + stride * lax.broadcasted_iota(jnp.int32, (count, 128), 0) + shift
    mass = (lane >= 64) & (lane < 68)
    tail = piece[:, 256:384].astype(F32)
    dead = jnp.where(mass & (position >= valid), MASKED, 0.0)
    ka[at, :128] = piece[:, :128]
    ka[at, 128:256] = jnp.where(lane < 64, tail, dead).astype(BF16)
    va[at, :128] = piece[:, 128:256]
    va[at, 128:256] = jnp.where(
        lane < 64, pltpu.roll(tail, 64, 1), jnp.where(mass, 1.0, 0.0)
    ).astype(BF16)


def merge(old, new, peak, h):
    before = old[1][:, 68 + h : 69 + h]
    top = jnp.maximum(before, peak)
    keep = jnp.exp2(before - top)
    add = jnp.exp2(peak - top)
    first = jnp.where(head_tile_all(h, 0), keep * old[0] + add * new[0], old[0])
    second = jnp.where(head_tile(h, 1), keep * old[1] + add * new[1], old[1])
    second = jnp.where(lanes() == 68 + h, top, second)
    return first, second


def normalised(first, second):
    lane = lanes()
    inv = [1.0 / second[:, 64 + h : 65 + h] for h in range(4)]
    one = first * jnp.where(lane < HS, inv[0], jnp.where(lane < 2 * HS, inv[1], inv[2]))
    two = second * jnp.where(lane < 16, inv[2], inv[3])
    return one, two


def packed(one, two):
    half = two.shape[0] // 2
    tail = jnp.where(lanes() < 64, two[:half], pltpu.roll(two[half:], 64, 1))
    return one.astype(BF16), tail.astype(BF16)


def middle_kernel(tok_rows, scal, offs, acc_ref, qm_ref, own_ref, far_ref, swap_ref,
                  out_ref, accw_ref, ka, va, a0, a1):
    seq = scal[2]
    count = own_ref.shape[0]
    sources = (seq, seq ^ 2, seq ^ 1, seq ^ 3)
    pieces = (own_ref[...], far_ref[...], swap_ref[:count], swap_ref[count:])
    for i, (source, piece) in enumerate(zip(sources, pieces)):
        open_piece(piece, source * tok_rows, R1, offs, 0, scal[1], ka, va, slice(i * count, (i + 1) * count))
    a0[...] = acc_ref[0]
    a1[...] = acc_ref[1]
    for h in range(4):
        peak, out = attend(qm_ref[h * count : (h + 1) * count], ka[...], va[...])
        at = pl.ds(offs[0, h], count, stride=R1)
        first, second = merge((a0[at, :], a1[at, :]), (out[:, :128], out[:, 128:]), peak, h)
        a0[at, :] = first
        a1[at, :] = second
    wide = accw_ref.shape[1]
    first = jnp.zeros((wide, 128), F32)
    second = jnp.zeros((wide, 128), F32)
    for h in range(4):
        at = pl.ds(offs[1, h], wide, stride=R2)
        first = jnp.where(head_tile_all(h, 0), a0[at, :], first)
        second = jnp.where(head_tile_all(h, 1), a1[at, :], second)
    accw_ref[0] = first
    accw_ref[1] = second
    one, two = normalised(a0[...], a1[...])
    head, tail = packed(one, two)
    out_ref[: head.shape[0]] = head
    out_ref[head.shape[0] :] = tail


Z_NEAR = (0, -1, 1, -2)
Z_FAR = (0, -4, 4, 8)


def wide_kernel(tok_rows, n_chips, scal, offs, qw_ref, own_ref, swap_ref, accw_ref, out_ref, ka, va):
    chip, core = scal[2] // 2, scal[2] % 2
    count = qw_ref.shape[0] // 4
    at = 0
    for side, ref in ((core, own_ref), (1 - core, swap_ref)):
        base = 0
        for near in Z_NEAR:
            for far in Z_FAR:
                source = lax.rem(chip + (near + far) + 2 * n_chips, n_chips) * 2 + side
                open_piece(ref[base : base + count], source * tok_rows, R2, offs, 1, scal[1],
                           ka, va, slice(at, at + count))
                base += count
                at += count
    peak, out = attend(qw_ref[...], ka[...], va[...])
    first, second = accw_ref[0], accw_ref[1]
    for h in range(4):
        rows = slice(h * count, (h + 1) * count)
        first, second = merge((first, second), (out[rows, :128], out[rows, 128:]), peak[rows], h)
    one, two = normalised(first, second)
    head, tail = packed(one, two)
    out_ref[:count] = head
    out_ref[count:] = tail


def final_kernel(scal, offs, w_ref, a0_ref, a1_ref, a2_ref, a3_ref, b0_ref, b1_ref, b2_ref, b3_ref,
                 out_ref, f0, f1, xs):
    rows = out_ref.shape[0]
    half = rows // 2
    sub, subs = scal[3], 4
    count = rows // R2
    for i, (a_ref, b_ref) in enumerate(((a0_ref, b0_ref), (a1_ref, b1_ref), (a2_ref, b2_ref), (a3_ref, b3_ref))):
        source = lax.rem(sub + (0, subs - 1, 1, 2)[i], subs)
        f0[...] = a_ref[:rows].astype(F32)
        tail = a_ref[rows:].astype(F32)
        f1[:half] = tail
        f1[half:] = pltpu.roll(tail, 64, 1)
        b0 = b_ref[:count].astype(F32)
        tail = b_ref[count:].astype(F32)
        b1 = jnp.concatenate([tail, pltpu.roll(tail, 64, 1)], axis=0)
        for h in range(4):
            at = pl.ds(offs[1, source * 4 + h], count, stride=R2)
            if h < 3:
                f0[at, :] = jnp.where(head_tile_all(h, 0), b0, f0[at, :])
            if h > 1:
                f1[at, :] = jnp.where(head_tile_all(h, 1), b1, f1[at, :])
        xs[:, i * 256 : i * 256 + 128] = f0[...].astype(BF16)
        xs[:, i * 256 + 128 : (i + 1) * 256] = f1[...].astype(BF16)
    chunk = 256

    def step(i, carry):
        start = pl.multiple_of(i * chunk, chunk)
        at = pl.ds(start, chunk)
        total = jnp.zeros((chunk, out_ref.shape[1]), F32)
        for j in range(4):
            source = lax.rem(sub + (0, subs - 1, 1, 2)[j], subs)
            total += jnp.dot(xs[at, j * 256 : (j + 1) * 256], w_ref[source], preferred_element_type=F32)
        position = scal[0] + start + lax.broadcasted_iota(jnp.int32, (chunk, 1), 0)
        out_ref[at, :] = jnp.where(position < scal[1], total, 0.0).astype(BF16)
        return carry

    lax.fori_loop(0, rows // chunk, step, 0)


def call(body, outs, scratch, n_smem, n_vmem, flops, name):
    return pl.pallas_call(
        body,
        out_shape=[jax.ShapeDtypeStruct(s, d) for s, d in outs],
        in_specs=[SMEM] * n_smem + [VMEM] * n_vmem,
        out_specs=[VMEM] * len(outs),
        scratch_shapes=[pltpu.VMEM(s, d) for s, d in scratch],
        cost_estimate=pl.CostEstimate(flops=int(flops), bytes_accessed=2 << 20, transcendentals=0),
        name=name,
    )


def local(q_heads, k_heads, v_heads, w_out, offsets, valid):
    rows, cols = q_heads.shape
    seq = lax.axis_index("seq")
    sub = lax.axis_index("sub")
    n_seq = lax.axis_size("seq")
    n_sub = lax.axis_size("sub")
    n_chips = n_seq // 2
    mid, wide = rows // R1, rows // R2
    scal = jnp.stack([seq * rows, valid[0], seq, sub]).astype(jnp.int32)
    offs = lax.dynamic_slice_in_dim(offsets, sub * 4, 4, 1)
    w_cols = lax.dynamic_slice_in_dim(w_out, sub * cols, cols, 1).reshape(n_sub, cols, cols)
    w_cols = jnp.pad(w_cols, ((0, 0), (0, 256 - cols), (0, 0)))

    def along_z(value, step):
        pairs = [(2 * z + c, 2 * ((z + step) % n_chips) + c) for z in range(n_chips) for c in range(2)]
        return lax.ppermute(value, "seq", pairs)

    def flipped(value, mask):
        return lax.ppermute(value, "seq", [(i, i ^ mask) for i in range(n_seq)])

    def along_x(value, step):
        return lax.ppermute(value, "sub", [(i, (i + step) % n_sub) for i in range(n_sub)])

    kv_mid, kv_wide = call(
        prep_kernel,
        [((mid, 384), BF16), ((wide, 384), BF16)],
        [((rows, 128), F32)] * 4,
        1, 2, 2e8, "prep",
    )(offs, k_heads, v_heads)

    far_mid = flipped(kv_mid, 2)
    quarter = jnp.concatenate([kv_wide] + [along_z(kv_wide, -s) for s in Z_FAR[1:]], axis=0)
    acc, q_mid, q_wide = call(
        near_kernel,
        [((2, rows, 128), F32), ((4 * mid, 256), BF16), ((4 * wide, 256), BF16)],
        [((rows, 256), BF16)] * 3 + [((rows, 128), F32)] * 2,
        2, 3, 4e9, "near",
    )(scal, offs, q_heads, k_heads, v_heads)
    swap_mid = flipped(jnp.concatenate([kv_mid, far_mid], axis=0), 1)
    attn, acc_wide = call(
        functools.partial(middle_kernel, rows),
        [((rows + rows // 2, 128), BF16), ((2, wide, 128), F32)],
        [((4 * mid, 256), BF16)] * 2 + [((rows, 128), F32)] * 2,
        2, 5, 1e9, "middle",
    )(scal, offs, acc, q_mid, kv_mid, far_mid, swap_mid)
    whole = jnp.concatenate([quarter] + [along_z(quarter, -s) for s in Z_NEAR[1:]], axis=0)
    other = flipped(whole, 1)
    attns = [attn] + [along_x(attn, s) for s in (1, n_sub - 1, 2)]
    (attn_wide,) = call(
        functools.partial(wide_kernel, rows, n_chips),
        [((wide + wide // 2, 128), BF16)],
        [((n_seq * wide, 256), BF16)] * 2,
        2, 4, 1e9, "wide",
    )(scal, offs, q_wide, whole, other, acc_wide)
    wides = [attn_wide] + [along_x(attn_wide, s) for s in (1, n_sub - 1, 2)]
    (out,) = call(
        final_kernel,
        [((rows, cols), BF16)],
        [((rows, 128), F32)] * 2 + [((rows, 1024), BF16)],
        2, 9, 1e9, "final",
    )(scal, offsets, w_cols, *attns, *wides)
    return out


def solution(mesh):
    placed = (
        P(("slides", "seq"), "sub"),
        P(("slides", "seq"), "sub"),
        P(("slides", "seq"), "sub"),
        P(),
        P(),
        P("slides"),
    )
    return jax.shard_map(
        local, mesh=mesh, in_specs=placed, out_specs=P(("slides", "seq"), "sub"), check_vma=False
    )
```

```python
import functools
import math

import jax
import jax.numpy as jnp
from jax import lax
from jax.experimental import pallas as pl
from jax.experimental.pallas import tpu as pltpu
from jax.sharding import PartitionSpec as P


HS = 48
R1 = 4
R2 = 16
LOG2_SCALE = HS ** (-0.5) * math.log2(math.e)
MASKED = -1e6

F32 = jnp.float32
BF16 = jnp.bfloat16


VMEM = pl.BlockSpec(memory_space=pltpu.VMEM)
SMEM = pl.BlockSpec(memory_space=pltpu.SMEM)


def lanes(width=128):
    return lax.broadcasted_iota(jnp.int32, (1, width), 1)


def head_lanes(h):
    lane = lanes(256)
    return ((lane >= h * HS) & (lane < (h + 1) * HS)) | (lane == 4 * HS + h)


def head_tile(h, tile):
    return head_lanes(h)[:, tile * 128 : (tile + 1) * 128]


def head_tile_all(h, tile):
    lane = lanes()
    if tile == 0:
        return (lane >= h * HS) & (lane < (h + 1) * HS)
    low = h * HS - 128
    return ((lane >= low) & (lane < low + HS) & (lane < 64)) | (lane == 64 + h) | (lane == 68 + h)


def attend(q, k, v, k_dims=(1,), v_dims=(0,)):
    scores = lax.dot_general(q, k, (((1,), k_dims), ((), ())), preferred_element_type=F32)
    peak = jnp.max(scores, axis=1, keepdims=True)
    probs = jnp.exp2((scores - peak) * LOG2_SCALE).astype(BF16)
    out = lax.dot_general(probs, v, (((1,), v_dims), ((), ())), preferred_element_type=F32)
    return peak * LOG2_SCALE, out


def prep_kernel(offs_hbm, k_hbm, v_hbm, mid_ref, wide_ref, k_ref, v_ref, offsets, kf, vf, tf, sems):
    copies = [
        pltpu.make_async_copy(source, target, sems.at[i])
        for i, (source, target) in enumerate(
            ((offs_hbm, offsets), (k_hbm, k_ref), (v_hbm, v_ref))
        )
    ]
    for copy in copies:
        copy.start()
    first_head = lax.axis_index("sub") * 4
    copies[1].wait()
    kf[...] = k_ref[:128, :].astype(F32).T
    copies[2].wait()
    vf[...] = v_ref[:128, :].astype(F32).T
    tf[...] = jnp.concatenate([k_ref[128:192, :], v_ref[128:192, :]], axis=0).astype(F32).T
    copies[0].wait()
    lane = lanes()
    for row, stride, out in ((0, R1, mid_ref), (1, R2, wide_ref)):
        count = out.shape[0]

        def pick(ref, h):
            return ref[pl.ds(offsets[row, first_head + h], count, stride=stride), :]

        for tile, ref in ((0, kf), (1, vf)):
            joined = jnp.where(lane < HS, pick(ref, 0), jnp.where(lane < 2 * HS, pick(ref, 1), pick(ref, 2)))
            out[:, tile * 128 : (tile + 1) * 128] = joined.astype(BF16)
        joined = jnp.where(lane % 64 < 16, pick(tf, 2), pick(tf, 3))
        out[:, 256:384] = joined.astype(BF16)


def near_kernel(valid, offs_hbm, q_ref, k_ref, v_ref, acc_ref, qm_ref, qw_ref, qa, ka, va, q0, q1, offsets, sem):
    rows = q_ref.shape[1]
    fetch = pltpu.make_async_copy(offs_hbm, offsets, sem)
    fetch.start()
    first_head = lax.axis_index("sub") * 4
    start = lax.axis_index("seq") * rows
    line = lax.broadcasted_iota(jnp.int32, (64, 1), 0)
    ones = jnp.broadcast_to(jnp.where(line < 4, 1.0, 0.0), (64, rows))
    q0[...] = q_ref[:128, :].astype(F32).T
    q1[...] = jnp.concatenate([q_ref[128:192, :].astype(F32), ones], axis=0).T
    qa[:, :128] = q0[...].astype(BF16)
    qa[:, 128:256] = q1[...].astype(BF16)
    position = start + lax.broadcasted_iota(jnp.int32, (1, rows), 1)
    dead = jnp.where(position < valid[0], 0.0, MASKED)
    ka[:192, :] = k_ref[...]
    ka[192:256, :] = jnp.where(line < 4, dead, 0.0).astype(BF16)
    va[:192, :] = v_ref[...]
    va[192:256, :] = ones.astype(BF16)
    fetch.wait()

    for row, stride, out in ((0, R1, qm_ref), (1, R2, qw_ref)):
        count = rows // stride
        for h in range(4):
            for tile, ref in ((0, q0), (1, q1)):
                picked = ref[pl.ds(offsets[row, first_head + h], count, stride=stride), :]
                picked = jnp.where(head_tile(h, tile), picked, 0.0)
                out[h * count : (h + 1) * count, tile * 128 : (tile + 1) * 128] = picked.astype(BF16)

    chunk = 512

    def step(i, carry):
        at = pl.ds(pl.multiple_of(i * chunk, chunk), chunk)
        q = qa[at, :]

        def score(h):
            qh = jnp.where(head_lanes(h), q, jnp.zeros((), BF16))
            return jnp.dot(qh, ka[...], preferred_element_type=F32)

        acc = jnp.zeros((chunk, 256), F32)
        later = score(0)
        for h in range(4):
            scores = later
            if h < 3:
                later = score(h + 1)
            peak = jnp.max(scores, axis=1, keepdims=True)
            probs = jnp.exp2((scores - peak) * LOG2_SCALE).astype(BF16)
            out = lax.dot_general(probs, va[...], (((1,), (1,)), ((), ())), preferred_element_type=F32)
            acc = jnp.where(head_lanes(h), out, acc)
            acc = jnp.where(lanes(256) == 4 * HS + 4 + h, peak * LOG2_SCALE, acc)
        acc_ref[0, at, :] = acc[:, :128]
        acc_ref[1, at, :] = acc[:, 128:]
        return carry

    lax.fori_loop(0, rows // chunk, step, 0)


def open_piece(piece, first, stride, offsets, row, valid, ka, va, at):
    count = piece.shape[0]
    first_head = lax.axis_index("sub") * 4
    lane = lanes()
    shift = jnp.zeros((1, 128), jnp.int32)
    for h in range(4):
        shift = jnp.where(lane == 64 + h, offsets[row, first_head + h], shift)
    position = first + stride * lax.broadcasted_iota(jnp.int32, (count, 128), 0) + shift
    mass = (lane >= 64) & (lane < 68)
    tail = piece[:, 256:384].astype(F32)
    dead = jnp.where(mass & (position >= valid[0]), MASKED, 0.0)
    ka[at, :128] = piece[:, :128]
    ka[at, 128:256] = jnp.where(lane < 64, tail, dead).astype(BF16)
    va[at, :128] = piece[:, 128:256]
    va[at, 128:256] = jnp.where(
        lane < 64, pltpu.roll(tail, 64, 1), jnp.where(mass, 1.0, 0.0)
    ).astype(BF16)


def merge(old, new, peak, h):
    before = old[1][:, 68 + h : 69 + h]
    top = jnp.maximum(before, peak)
    keep = jnp.exp2(before - top)
    add = jnp.exp2(peak - top)
    first = jnp.where(head_tile_all(h, 0), keep * old[0] + add * new[0], old[0]) if h < 3 else old[0]
    second = jnp.where(head_tile(h, 1), keep * old[1] + add * new[1], old[1])
    second = jnp.where(lanes() == 68 + h, top, second)
    return first, second


def normalised(first, second):
    lane = lanes()
    inv = [1.0 / second[:, 64 + h : 65 + h] for h in range(4)]
    one = first * jnp.where(lane < HS, inv[0], jnp.where(lane < 2 * HS, inv[1], inv[2]))
    two = second * jnp.where(lane < 16, inv[2], inv[3])
    return one, two


def packed(one, two):
    half = two.shape[0] // 2
    tail = jnp.where(lanes() < 64, two[:half], pltpu.roll(two[half:], 64, 1))
    return one.astype(BF16), tail.astype(BF16)


def middle_kernel(tok_rows, offsets, valid, acc_ref, qm_ref, own_ref, far_ref, swap_ref,
                  out_ref, accw_ref, ka, va, a0, a1):
    seq = lax.axis_index("seq")
    first_head = lax.axis_index("sub") * 4
    count = own_ref.shape[0]
    sources = (seq, seq ^ 2, seq ^ 1, seq ^ 3)
    pieces = (own_ref[...], far_ref[...], swap_ref[:count], swap_ref[count:])
    for i, (source, piece) in enumerate(zip(sources, pieces)):
        open_piece(piece, source * tok_rows, R1, offsets, 0, valid, ka, va, slice(i * count, (i + 1) * count))
    a0[...] = acc_ref[0]
    a1[...] = acc_ref[1]
    for h in range(4):
        peak, out = attend(qm_ref[h * count : (h + 1) * count], ka[...], va[...])
        at = pl.ds(offsets[0, first_head + h], count, stride=R1)
        first, second = merge((a0[at, :], a1[at, :]), (out[:, :128], out[:, 128:]), peak, h)
        if h < 3:
            a0[at, :] = first
        a1[at, :] = second
    wide = accw_ref.shape[1]
    first = jnp.zeros((wide, 128), F32)
    second = jnp.zeros((wide, 128), F32)
    for h in range(4):
        at = pl.ds(offsets[1, first_head + h], wide, stride=R2)
        here0, here1 = a0[at, :], a1[at, :]
        first = jnp.where(head_tile_all(h, 0), here0, first)
        second = jnp.where(head_tile_all(h, 1), here1, second)
        if h < 3:
            a0[at, :] = jnp.where(head_tile_all(h, 0), 0.0, here0)
        if h > 1:
            a1[at, :] = jnp.where(head_tile_all(h, 1) & (lanes() < 64), 0.0, here1)
    accw_ref[0] = first
    accw_ref[1] = second
    one, two = normalised(a0[...], a1[...])
    head, tail = packed(one, two)
    out_ref[: head.shape[0]] = head
    out_ref[head.shape[0] :] = tail


def gathered_from(n_chips, side, group):
    chip = lax.axis_index("seq") // 2
    ahead = 2 * side - 1
    four, eight = n_chips // 4, n_chips // 2
    pieces = []
    for step in ((0,), (-1, 1))[group]:
        pieces += [(step, side), (step + four * ahead, side), (step + four * ahead, 1 - side), (step + eight, side)]
    if group == 0:
        for step in (2 * ahead, (2 + four) * ahead):
            pieces += [(step, side), (step, 1 - side)]
    return [(lax.rem(chip + step + n_chips, n_chips), core) for step, core in pieces]


def wide_kernel(tok_rows, n_chips, plan, last, offsets, valid, qw_ref, accw_ref, *refs):
    keys, (out_ref, ka, va) = refs[: len(plan)], refs[len(plan) :]
    core = lax.rem(lax.axis_index("seq"), 2)
    count = qw_ref.shape[0] // 4
    base = 0
    for (group, swapped), ref in zip(plan, keys):
        for i, (chip, core_of) in enumerate(gathered_from(n_chips, 1 - core if swapped else core, group)):
            at = slice(base, base + count)
            first = (chip * 2 + core_of) * tok_rows
            open_piece(ref[i * count : (i + 1) * count], first, R2, offsets, 1, valid, ka, va, at)
            base += count
    peak, out = attend(qw_ref[...], ka[...], va[...])
    first, second = accw_ref[0], accw_ref[1]
    for h in range(4):
        rows = slice(h * count, (h + 1) * count)
        first, second = merge((first, second), (out[rows, :128], out[rows, 128:]), peak[rows], h)
    if not last:
        out_ref[0] = first
        out_ref[1] = second
        return
    head, tail = packed(*normalised(first, second))
    out_ref[:count] = head
    out_ref[count:] = tail


X_FROM = (0, -1, 1, 2)


def x_sources():
    sub, subs = lax.axis_index("sub"), lax.axis_size("sub")
    return [lax.rem(sub + step + subs, subs) for step in X_FROM]


def final_kernel(offsets, valid, w_ref, a0_ref, a1_ref, a2_ref, a3_ref, b0_ref, b1_ref, b2_ref, b3_ref,
                 out_ref, f0, f1, wp):
    cols, rows = out_ref.shape
    half, count, chunk = rows // 2, rows // R2, 256
    sources = x_sources()
    wp[...] = jnp.zeros(wp.shape, BF16)
    for i, source in enumerate(sources):
        at = pl.ds(pl.multiple_of(source * cols, cols), cols)
        for part in (0, 1):
            for low, high in ((0, 128), (128, cols)):
                piece = w_ref[at, low:high]
                wp[part, i * 256 : i * 256 + 128, low:high] = piece[:128]
                tail = i * 256 + 128 + part * 64
                wp[part, tail : tail + 64, low:high] = piece[128:]
    for part in (0, 1):
        for start in range(0, half, chunk):
            at = slice(part * half + start, part * half + start + chunk)
            tail = slice(rows + start, rows + start + chunk)
            x = jnp.concatenate(
                [piece for ref in (a0_ref, a1_ref, a2_ref, a3_ref) for piece in (ref[at], ref[tail])], axis=1
            )
            total = jnp.dot(x, wp[part], preferred_element_type=F32)
            f0[at, :] = total[:, :128]
            f1[at, :] = total[:, 128:]
    for i, ref in enumerate((b0_ref, b1_ref, b2_ref, b3_ref)):
        tail = ref[count:].astype(F32)
        second = jnp.concatenate([tail, pltpu.roll(tail, 64, 1)], axis=0)
        both = jnp.concatenate([ref[:count].astype(F32), second], axis=1)
        stacked = jnp.concatenate(
            [jnp.where(head_lanes(h) & (lanes(256) < 4 * HS), both, 0.0) for h in range(4)], axis=0
        )
        part = jnp.dot(stacked.astype(BF16), wp[0, i * 256 : (i + 1) * 256], preferred_element_type=F32)
        for h in range(4):
            at = pl.ds(offsets[1, sources[i] * 4 + h], count, stride=R2)
            rows_h = slice(h * count, (h + 1) * count)
            f0[at, :] = f0[at, :] + part[rows_h, :128]
            f1[at, :] = f1[at, :] + part[rows_h, 128:]
    position = lax.axis_index("seq") * rows + lax.broadcasted_iota(jnp.int32, (1, rows), 1)
    keep = position < valid[0]
    out_ref[:128, :] = jnp.where(keep, f0[...].T, 0.0).astype(BF16)
    out_ref[128:, :] = jnp.where(keep, f1[...].T[: cols - 128], 0.0).astype(BF16)


HBM = pl.BlockSpec(memory_space=pltpu.HBM)


def call(body, ins, outs, scratch, flops, limit=20):
    return pl.pallas_call(
        body,
        out_shape=[jax.ShapeDtypeStruct(s, d) for s, d in outs],
        in_specs=[{"s": SMEM, "v": VMEM, "a": HBM}[kind] for kind in ins],
        out_specs=[VMEM] * len(outs),
        scratch_shapes=[s if not isinstance(s, tuple) else pltpu.VMEM(*s) for s in scratch],
        cost_estimate=pl.CostEstimate(flops=int(flops), bytes_accessed=2 << 20, transcendentals=0),
        compiler_params=pltpu.CompilerParams(vmem_limit_bytes=limit << 20),
    )


def local(q_heads, k_heads, v_heads, w_out, offsets, valid):
    rows, cols = q_heads.shape
    sub = lax.axis_index("sub")
    n_seq = lax.axis_size("seq")
    n_sub = lax.axis_size("sub")
    n_chips = n_seq // 2
    mid, wide = rows // R1, rows // R2
    w_cols = lax.dynamic_slice_in_dim(w_out, sub * cols, cols, 1)

    def along_z(value, up, down):
        pairs = [(2 * z + c, 2 * ((z + (up, down)[c]) % n_chips) + c) for z in range(n_chips) for c in (0, 1)]
        return lax.ppermute(value, "seq", pairs)

    def flipped(value, mask):
        return lax.ppermute(value, "seq", [(i, i ^ mask) for i in range(n_seq)])

    def along_x(value, step):
        return lax.ppermute(value, "sub", [(i, (i + step) % n_sub) for i in range(n_sub)])

    smem_offsets = pltpu.SMEM(offsets.shape, jnp.int32)
    q_t, k_t, v_t = q_heads.T, k_heads.T, v_heads.T
    kv_mid, kv_wide = call(
        prep_kernel, "aaa",
        [((mid, 384), BF16), ((wide, 384), BF16)],
        [((cols, rows), BF16)] * 2 + [smem_offsets] + [((rows, 128), F32)] * 3 + [pltpu.SemaphoreType.DMA((3,))],
        2e8, 60,
    )(offsets, k_t, v_t)

    four = n_chips // 4
    kv_both = flipped(kv_wide, 1)
    far_mid = flipped(kv_mid, 2)
    own_pair = jnp.concatenate([kv_wide, kv_both], axis=0)
    far4 = along_z(own_pair, four, -four)
    acc, q_mid, q_wide = call(
        near_kernel, "savvv",
        [((2, rows, 128), F32), ((4 * mid, 256), BF16), ((4 * wide, 256), BF16)],
        [((rows, 256), BF16), ((256, rows), BF16), ((256, rows), BF16)] + [((rows, 128), F32)] * 2
        + [smem_offsets, pltpu.SemaphoreType.DMA],
        4e9, 28,
    )(valid, offsets, q_t, k_t, v_t)
    far_mid, acc = lax.optimization_barrier((far_mid, acc))

    swap_mid = flipped(jnp.concatenate([kv_mid, far_mid], axis=0), 1)
    far8 = along_z(far4[:wide], four, -four)
    mine = jnp.concatenate([kv_wide, far4, far8], axis=0)
    around2 = along_z(jnp.concatenate([own_pair, far4], axis=0), 2, -2)
    around_up = along_z(mine, 1, 1)
    around_down = along_z(mine, -1, -1)
    attn, acc_wide = call(
        functools.partial(middle_kernel, rows), "ssvvvvv",
        [((rows + rows // 2, 128), BF16), ((2, wide, 128), F32)],
        [((4 * mid, 256), BF16)] * 2 + [((rows, 128), F32)] * 2,
        1e9,
    )(offsets, valid, acc, q_mid, kv_mid, far_mid, swap_mid)
    attns = [along_x(attn, s) for s in (1, n_sub - 1, 2)]

    def wide_part(plan, acc_now, keys, last=False):
        n_keys = sum(k.shape[0] for k in keys)
        (result,) = call(
            functools.partial(wide_kernel, rows, n_chips, plan, last), "ssvv" + "v" * len(keys),
            [((wide + wide // 2, 128), BF16) if last else ((2, wide, 128), F32)],
            [((n_keys, 256), BF16)] * 2, 5e8,
        )(offsets, valid, q_wide, acc_now, *keys)
        return result

    early = jnp.concatenate([mine, around2], axis=0)
    early_other = flipped(early, 1)
    late = jnp.concatenate([around_up, around_down], axis=0)
    late_other = flipped(late, 1)
    acc_wide = wide_part(((0, False), (0, True)), acc_wide, (early, early_other))
    acc_wide = wide_part(((1, False),), acc_wide, (late,))
    attn_wide = wide_part(((1, True),), acc_wide, (late_other,), last=True)
    wides = [along_x(attn_wide, s) for s in (1, n_sub - 1, 2)]
    (out,) = call(
        final_kernel, "ssv" + "v" * 8, [((cols, rows), BF16)],
        [((rows, 128), F32)] * 2 + [((2, 4 * 256, 256), BF16)], 1e9,
    )(offsets, valid, w_cols, attn, *attns, attn_wide, *wides)
    return out.T


def solution(mesh):
    placed = (
        P(("slides", "seq"), "sub"),
        P(("slides", "seq"), "sub"),
        P(("slides", "seq"), "sub"),
        P(),
        P(),
        P("slides"),
    )


    return jax.shard_map(local, mesh=mesh, in_specs=placed, out_specs=P(("slides", "seq"), "sub"), check_vma=False)
```

```python
import functools
import math

import jax
import jax.numpy as jnp
from jax import lax
from jax.experimental import pallas as pl
from jax.experimental.pallas import tpu as pltpu
from jax.sharding import PartitionSpec as P


HS = 48
R1 = 4
R2 = 16
LOG2_SCALE = HS ** (-0.5) * math.log2(math.e)
MASKED = -1e6

F32 = jnp.float32
BF16 = jnp.bfloat16


VMEM = pl.BlockSpec(memory_space=pltpu.VMEM)
SMEM = pl.BlockSpec(memory_space=pltpu.SMEM)


def lanes(width=128):
    return lax.broadcasted_iota(jnp.int32, (1, width), 1)


def head_lanes(h):
    lane = lanes(256)
    return ((lane >= h * HS) & (lane < (h + 1) * HS)) | (lane == 4 * HS + h)


def head_tile(h, tile):
    return head_lanes(h)[:, tile * 128 : (tile + 1) * 128]


def head_tile_all(h, tile):
    lane = lanes()
    if tile == 0:
        return (lane >= h * HS) & (lane < (h + 1) * HS)
    low = h * HS - 128
    return ((lane >= low) & (lane < low + HS) & (lane < 64)) | (lane == 64 + h) | (lane == 68 + h)


def offset_of(code, row, h):
    return (code[0] >> (6 * h + 2 * row)) & (R1 - 1, R2 - 1)[row]


def attend(q, k, v, k_dims=(1,), v_dims=(0,)):
    scores = lax.dot_general(q, k, (((1,), k_dims), ((), ())), preferred_element_type=F32)
    peak = jnp.max(scores, axis=1, keepdims=True)
    probs = jnp.exp2((scores - peak) * LOG2_SCALE).astype(BF16)
    out = lax.dot_general(probs, v, (((1,), v_dims), ((), ())), preferred_element_type=F32)
    return peak * LOG2_SCALE, out


def prep_kernel(offs_hbm, k_hbm, v_hbm, mid_ref, wide_ref, k_ref, v_ref, offsets, kf, vf, tf, sems):
    copies = [
        pltpu.make_async_copy(source, target, sems.at[i])
        for i, (source, target) in enumerate(
            ((offs_hbm, offsets), (k_hbm, k_ref), (v_hbm, v_ref))
        )
    ]
    for copy in copies:
        copy.start()
    first_head = lax.axis_index("sub") * 4
    copies[1].wait()
    kf[...] = k_ref[:128, :].astype(F32).T
    copies[2].wait()
    vf[...] = v_ref[:128, :].astype(F32).T
    tf[...] = jnp.concatenate([k_ref[128:192, :], v_ref[128:192, :]], axis=0).astype(F32).T
    copies[0].wait()
    lane = lanes()
    for row, stride, out in ((0, R1, mid_ref), (1, R2, wide_ref)):
        count = out.shape[0]

        def pick(ref, h):
            return ref[pl.ds(offsets[row, first_head + h], count, stride=stride), :]

        for tile, ref in ((0, kf), (1, vf)):
            joined = jnp.where(lane < HS, pick(ref, 0), jnp.where(lane < 2 * HS, pick(ref, 1), pick(ref, 2)))
            out[:, tile * 128 : (tile + 1) * 128] = joined.astype(BF16)
        joined = jnp.where(lane % 64 < 16, pick(tf, 2), pick(tf, 3))
        out[:, 256:384] = joined.astype(BF16)


def near_kernel(code, valid, q_ref, k_ref, v_ref, acc_ref, qm_ref, qw_ref, qa, ka, va, q0, q1):
    rows = q_ref.shape[1]
    start = lax.axis_index("seq") * rows
    line = lax.broadcasted_iota(jnp.int32, (64, 1), 0)
    ones = jnp.broadcast_to(jnp.where(line < 4, 1.0, 0.0), (64, rows))
    q0[...] = q_ref[:128, :].astype(F32).T
    q1[...] = jnp.concatenate([q_ref[128:192, :].astype(F32), ones], axis=0).T
    qa[:, :128] = q0[...].astype(BF16)
    qa[:, 128:256] = q1[...].astype(BF16)
    position = start + lax.broadcasted_iota(jnp.int32, (1, rows), 1)
    dead = jnp.where(position < valid[0], 0.0, MASKED)
    ka[:192, :] = k_ref[...]
    ka[192:256, :] = jnp.where(line < 4, dead, 0.0).astype(BF16)
    va[:192, :] = v_ref[...]
    va[192:256, :] = ones.astype(BF16)

    for row, stride, out in ((0, R1, qm_ref), (1, R2, qw_ref)):
        count = rows // stride
        for h in range(4):
            for tile, ref in ((0, q0), (1, q1)):
                picked = ref[pl.ds(offset_of(code, row, h), count, stride=stride), :]
                picked = jnp.where(head_tile(h, tile), picked, 0.0)
                out[h * count : (h + 1) * count, tile * 128 : (tile + 1) * 128] = picked.astype(BF16)

    chunk = 512

    def step(i, carry):
        at = pl.ds(pl.multiple_of(i * chunk, chunk), chunk)
        q = qa[at, :]

        def score(h):
            qh = jnp.where(head_lanes(h), q, jnp.zeros((), BF16))
            return jnp.dot(qh, ka[...], preferred_element_type=F32)

        acc = jnp.zeros((chunk, 256), F32)
        later = score(0)
        for h in range(4):
            scores = later
            if h < 3:
                later = score(h + 1)
            peak = jnp.max(scores, axis=1, keepdims=True)
            probs = jnp.exp2((scores - peak) * LOG2_SCALE).astype(BF16)
            out = lax.dot_general(probs, va[...], (((1,), (1,)), ((), ())), preferred_element_type=F32)
            acc = jnp.where(head_lanes(h), out, acc)
            acc = jnp.where(lanes(256) == 4 * HS + 4 + h, peak * LOG2_SCALE, acc)
        acc_ref[0, at, :] = acc[:, :128]
        acc_ref[1, at, :] = acc[:, 128:]
        return carry

    lax.fori_loop(0, rows // chunk, step, 0)


def open_piece(piece, first, stride, code, row, valid, ka, va, at):
    count = piece.shape[0]
    lane = lanes()
    shift = jnp.zeros((1, 128), jnp.int32)
    for h in range(4):
        shift = jnp.where(lane == 64 + h, offset_of(code, row, h), shift)
    position = first + stride * lax.broadcasted_iota(jnp.int32, (count, 128), 0) + shift
    mass = (lane >= 64) & (lane < 68)
    tail = piece[:, 256:384].astype(F32)
    dead = jnp.where(mass & (position >= valid[0]), MASKED, 0.0)
    ka[at, :128] = piece[:, :128]
    ka[at, 128:256] = jnp.where(lane < 64, tail, dead).astype(BF16)
    va[at, :128] = piece[:, 128:256]
    va[at, 128:256] = jnp.where(
        lane < 64, pltpu.roll(tail, 64, 1), jnp.where(mass, 1.0, 0.0)
    ).astype(BF16)


def merge(old, new, peak, h):
    before = old[1][:, 68 + h : 69 + h]
    top = jnp.maximum(before, peak)
    keep = jnp.exp2(before - top)
    add = jnp.exp2(peak - top)
    first = jnp.where(head_tile_all(h, 0), keep * old[0] + add * new[0], old[0]) if h < 3 else old[0]
    second = jnp.where(head_tile(h, 1), keep * old[1] + add * new[1], old[1])
    second = jnp.where(lanes() == 68 + h, top, second)
    return first, second


def normalised(first, second):
    lane = lanes()
    inv = [1.0 / second[:, 64 + h : 65 + h] for h in range(4)]
    one = first * jnp.where(lane < HS, inv[0], jnp.where(lane < 2 * HS, inv[1], inv[2]))
    two = second * jnp.where(lane < 16, inv[2], inv[3])
    return one, two


def packed(one, two):
    half = two.shape[0] // 2
    tail = jnp.where(lanes() < 64, two[:half], pltpu.roll(two[half:], 64, 1))
    return one.astype(BF16), tail.astype(BF16)


def middle_kernel(tok_rows, code, valid, acc_ref, qm_ref, own_ref, far_ref, swap_ref,
                  out_ref, accw_ref, ka, va, a0, a1):
    seq = lax.axis_index("seq")
    count = own_ref.shape[0]
    sources = (seq, seq ^ 2, seq ^ 1, seq ^ 3)
    pieces = (own_ref[...], far_ref[...], swap_ref[:count], swap_ref[count:])
    for i, (source, piece) in enumerate(zip(sources, pieces)):
        open_piece(piece, source * tok_rows, R1, code, 0, valid, ka, va, slice(i * count, (i + 1) * count))
    a0[...] = acc_ref[0]
    a1[...] = acc_ref[1]
    for h in range(4):
        peak, out = attend(qm_ref[h * count : (h + 1) * count], ka[...], va[...])
        at = pl.ds(offset_of(code, 0, h), count, stride=R1)
        first, second = merge((a0[at, :], a1[at, :]), (out[:, :128], out[:, 128:]), peak, h)
        if h < 3:
            a0[at, :] = first
        a1[at, :] = second
    wide = accw_ref.shape[1]
    first = jnp.zeros((wide, 128), F32)
    second = jnp.zeros((wide, 128), F32)
    for h in range(4):
        at = pl.ds(offset_of(code, 1, h), wide, stride=R2)
        here0, here1 = a0[at, :], a1[at, :]
        first = jnp.where(head_tile_all(h, 0), here0, first)
        second = jnp.where(head_tile_all(h, 1), here1, second)
        if h < 3:
            a0[at, :] = jnp.where(head_tile_all(h, 0), 0.0, here0)
        if h > 1:
            a1[at, :] = jnp.where(head_tile_all(h, 1) & (lanes() < 64), 0.0, here1)
    accw_ref[0] = first
    accw_ref[1] = second
    one, two = normalised(a0[...], a1[...])
    head, tail = packed(one, two)
    out_ref[: head.shape[0]] = head
    out_ref[head.shape[0] :] = tail


def gathered_from(n_chips, side, group):
    chip = lax.axis_index("seq") // 2
    ahead = 2 * side - 1
    four, eight = n_chips // 4, n_chips // 2
    pieces = []
    for step in ((0,), (-1, 1))[group]:
        pieces += [(step, side), (step + four * ahead, side), (step + four * ahead, 1 - side), (step + eight, side)]
    if group == 0:
        for step in (2 * ahead, (2 + four) * ahead):
            pieces += [(step, side), (step, 1 - side)]
    return [(lax.rem(chip + step + n_chips, n_chips), core) for step, core in pieces]


def wide_kernel(tok_rows, n_chips, plan, last, code, valid, qw_ref, accw_ref, *refs):
    keys, (out_ref, ka, va) = refs[: len(plan)], refs[len(plan) :]
    core = lax.rem(lax.axis_index("seq"), 2)
    count = qw_ref.shape[0] // 4
    base = 0
    for (group, swapped), ref in zip(plan, keys):
        for i, (chip, core_of) in enumerate(gathered_from(n_chips, 1 - core if swapped else core, group)):
            at = slice(base, base + count)
            first = (chip * 2 + core_of) * tok_rows
            open_piece(ref[i * count : (i + 1) * count], first, R2, code, 1, valid, ka, va, at)
            base += count
    peak, out = attend(qw_ref[...], ka[...], va[...])
    first, second = accw_ref[0], accw_ref[1]
    for h in range(4):
        rows = slice(h * count, (h + 1) * count)
        first, second = merge((first, second), (out[rows, :128], out[rows, 128:]), peak[rows], h)
    if not last:
        out_ref[0] = first
        out_ref[1] = second
        return
    head, tail = packed(*normalised(first, second))
    out_ref[:count] = head
    out_ref[count:] = tail


X_FROM = (0, -1, 1, 2)


def x_sources():
    sub, subs = lax.axis_index("sub"), lax.axis_size("sub")
    return [lax.rem(sub + step + subs, subs) for step in X_FROM]


def final_kernel(offs_hbm, valid, w_ref, a0_ref, a1_ref, a2_ref, a3_ref, b0_ref, b1_ref, b2_ref, b3_ref,
                 out_ref, f0, f1, wp, offsets, sem):
    cols, rows = out_ref.shape
    fetch = pltpu.make_async_copy(offs_hbm, offsets, sem)
    fetch.start()
    half, count, chunk = rows // 2, rows // R2, 256
    sources = x_sources()
    wp[...] = jnp.zeros(wp.shape, BF16)
    for i, source in enumerate(sources):
        at = pl.ds(pl.multiple_of(source * cols, cols), cols)
        for part in (0, 1):
            for low, high in ((0, 128), (128, cols)):
                piece = w_ref[at, low:high]
                wp[part, i * 256 : i * 256 + 128, low:high] = piece[:128]
                tail = i * 256 + 128 + part * 64
                wp[part, tail : tail + 64, low:high] = piece[128:]
    for part in (0, 1):
        for start in range(0, half, chunk):
            at = slice(part * half + start, part * half + start + chunk)
            tail = slice(rows + start, rows + start + chunk)
            x = jnp.concatenate(
                [piece for ref in (a0_ref, a1_ref, a2_ref, a3_ref) for piece in (ref[at], ref[tail])], axis=1
            )
            total = jnp.dot(x, wp[part], preferred_element_type=F32)
            f0[at, :] = total[:, :128]
            f1[at, :] = total[:, 128:]
    fetch.wait()
    for i, ref in enumerate((b0_ref, b1_ref, b2_ref, b3_ref)):
        tail = ref[count:].astype(F32)
        second = jnp.concatenate([tail, pltpu.roll(tail, 64, 1)], axis=0)
        both = jnp.concatenate([ref[:count].astype(F32), second], axis=1)
        stacked = jnp.concatenate(
            [jnp.where(head_lanes(h) & (lanes(256) < 4 * HS), both, 0.0) for h in range(4)], axis=0
        )
        part = jnp.dot(stacked.astype(BF16), wp[0, i * 256 : (i + 1) * 256], preferred_element_type=F32)
        for h in range(4):
            at = pl.ds(offsets[1, sources[i] * 4 + h], count, stride=R2)
            rows_h = slice(h * count, (h + 1) * count)
            f0[at, :] = f0[at, :] + part[rows_h, :128]
            f1[at, :] = f1[at, :] + part[rows_h, 128:]
    position = lax.axis_index("seq") * rows + lax.broadcasted_iota(jnp.int32, (1, rows), 1)
    keep = position < valid[0]
    out_ref[:128, :] = jnp.where(keep, f0[...].T, 0.0).astype(BF16)
    out_ref[128:, :] = jnp.where(keep, f1[...].T[: cols - 128], 0.0).astype(BF16)


HBM = pl.BlockSpec(memory_space=pltpu.HBM)


def call(body, ins, outs, scratch, flops, limit=20):
    return pl.pallas_call(
        body,
        out_shape=[jax.ShapeDtypeStruct(s, d) for s, d in outs],
        in_specs=[{"s": SMEM, "v": VMEM, "a": HBM}[kind] for kind in ins],
        out_specs=[VMEM] * len(outs),
        scratch_shapes=[s if not isinstance(s, tuple) else pltpu.VMEM(*s) for s in scratch],
        cost_estimate=pl.CostEstimate(flops=int(flops), bytes_accessed=2 << 20, transcendentals=0),
        compiler_params=pltpu.CompilerParams(vmem_limit_bytes=limit << 20),
    )


def local(q_heads, k_heads, v_heads, w_out, offsets, valid):
    rows, cols = q_heads.shape
    sub = lax.axis_index("sub")
    n_seq = lax.axis_size("seq")
    n_sub = lax.axis_size("sub")
    n_chips = n_seq // 2
    mid, wide = rows // R1, rows // R2
    shifts = 6 * lax.broadcasted_iota(jnp.int32, (2, 4), 1) + 2 * lax.broadcasted_iota(jnp.int32, (2, 4), 0)
    mine = lax.dynamic_slice_in_dim(offsets, sub * 4, 4, 1)
    code = (jnp.sum(jnp.left_shift(mine, shifts)) | (sub << 24)).reshape(1)
    w_cols = lax.dynamic_slice_in_dim(w_out, sub * cols, cols, 1)

    def along_z(value, up, down):
        pairs = [(2 * z + c, 2 * ((z + (up, down)[c]) % n_chips) + c) for z in range(n_chips) for c in (0, 1)]
        return lax.ppermute(value, "seq", pairs)

    def flipped(value, mask):
        return lax.ppermute(value, "seq", [(i, i ^ mask) for i in range(n_seq)])

    def along_x(value, step):
        return lax.ppermute(value, "sub", [(i, (i + step) % n_sub) for i in range(n_sub)])

    smem_offsets = pltpu.SMEM(offsets.shape, jnp.int32)
    q_t, k_t, v_t = q_heads.T, k_heads.T, v_heads.T
    near_q, w_cols = lax.optimization_barrier((q_t, w_cols))
    kv_mid, kv_wide = call(
        prep_kernel, "aaa",
        [((mid, 384), BF16), ((wide, 384), BF16)],
        [((cols, rows), BF16)] * 2 + [smem_offsets] + [((rows, 128), F32)] * 3 + [pltpu.SemaphoreType.DMA((3,))],
        2e8, 60,
    )(offsets, k_t, v_t)

    four = n_chips // 4
    kv_both = flipped(kv_wide, 1)
    far_mid = flipped(kv_mid, 2)
    own_pair = jnp.concatenate([kv_wide, kv_both], axis=0)
    far4 = along_z(own_pair, four, -four)
    acc, q_mid, q_wide = call(
        near_kernel, "ssvvv",
        [((2, rows, 128), F32), ((4 * mid, 256), BF16), ((4 * wide, 256), BF16)],
        [((rows, 256), BF16), ((256, rows), BF16), ((256, rows), BF16)] + [((rows, 128), F32)] * 2,
        4e9, 28,
    )(code, valid, near_q, k_t, v_t)
    far_mid, acc = lax.optimization_barrier((far_mid, acc))

    swap_mid = flipped(jnp.concatenate([kv_mid, far_mid], axis=0), 1)
    far8 = along_z(far4[:wide], four, -four)
    mine = jnp.concatenate([kv_wide, far4, far8], axis=0)
    around2 = along_z(jnp.concatenate([own_pair, far4], axis=0), 2, -2)
    around_up = along_z(mine, 1, 1)
    around_down = along_z(mine, -1, -1)
    attn, acc_wide = call(
        functools.partial(middle_kernel, rows), "ssvvvvv",
        [((rows + rows // 2, 128), BF16), ((2, wide, 128), F32)],
        [((4 * mid, 256), BF16)] * 2 + [((rows, 128), F32)] * 2,
        1e9,
    )(code, valid, acc, q_mid, kv_mid, far_mid, swap_mid)
    attns = [along_x(attn, s) for s in (1, n_sub - 1, 2)]

    def wide_part(plan, acc_now, keys, last=False):
        n_keys = sum(k.shape[0] for k in keys)
        (result,) = call(
            functools.partial(wide_kernel, rows, n_chips, plan, last), "ssvv" + "v" * len(keys),
            [((wide + wide // 2, 128), BF16) if last else ((2, wide, 128), F32)],
            [((n_keys, 256), BF16)] * 2, 5e8,
        )(code, valid, q_wide, acc_now, *keys)
        return result

    early = jnp.concatenate([mine, around2], axis=0)
    early_other = flipped(early, 1)
    late = jnp.concatenate([around_up, around_down], axis=0)
    late_other = flipped(late, 1)
    acc_wide = wide_part(((0, False), (0, True)), acc_wide, (early, early_other))
    acc_wide = wide_part(((1, False),), acc_wide, (late,))
    attn_wide = wide_part(((1, True),), acc_wide, (late_other,), last=True)
    wides = [along_x(attn_wide, s) for s in (1, n_sub - 1, 2)]
    (out,) = call(
        final_kernel, "asv" + "v" * 8, [((cols, rows), BF16)],
        [((rows, 128), F32)] * 2
        + [((2, 4 * 256, 256), BF16), smem_offsets, pltpu.SemaphoreType.DMA], 1e9,
    )(offsets, valid, w_cols, attn, *attns, attn_wide, *wides)
    return out.T


def solution(mesh):
    placed = (
        P(("slides", "seq"), "sub"),
        P(("slides", "seq"), "sub"),
        P(("slides", "seq"), "sub"),
        P(),
        P(),
        P("slides"),
    )


    return jax.shard_map(local, mesh=mesh, in_specs=placed, out_specs=P(("slides", "seq"), "sub"), check_vma=False)
```

```python
import functools
import math

import jax
import jax.numpy as jnp
from jax import lax
from jax.experimental import pallas as pl
from jax.experimental.pallas import tpu as pltpu
from jax.sharding import PartitionSpec as P


HS = 48
R1 = 4
R2 = 16
LOG2_SCALE = HS ** (-0.5) * math.log2(math.e)
MASKED = -1e6

F32 = jnp.float32
BF16 = jnp.bfloat16


VMEM = pl.BlockSpec(memory_space=pltpu.VMEM)
SMEM = pl.BlockSpec(memory_space=pltpu.SMEM)


def lanes(width=128):
    return lax.broadcasted_iota(jnp.int32, (1, width), 1)


def head_lanes(h):
    lane = lanes(256)
    return ((lane >= h * HS) & (lane < (h + 1) * HS)) | (lane == 4 * HS + h)


def head_tile(h, tile):
    return head_lanes(h)[:, tile * 128 : (tile + 1) * 128]


def head_tile_all(h, tile):
    lane = lanes()
    if tile == 0:
        return (lane >= h * HS) & (lane < (h + 1) * HS)
    low = h * HS - 128
    return ((lane >= low) & (lane < low + HS) & (lane < 64)) | (lane == 64 + h) | (lane == 68 + h)


def offset_of(code, row, h):
    return (code[0] >> (6 * h + 2 * row)) & (R1 - 1, R2 - 1)[row]


def attend(q, k, v, k_dims=(1,), v_dims=(0,)):
    scores = lax.dot_general(q, k, (((1,), k_dims), ((), ())), preferred_element_type=F32)
    peak = jnp.max(scores, axis=1, keepdims=True)
    probs = jnp.exp2((scores - peak) * LOG2_SCALE).astype(BF16)
    out = lax.dot_general(probs, v, (((1,), v_dims), ((), ())), preferred_element_type=F32)
    return peak * LOG2_SCALE, out


def prep_kernel(offs_hbm, k_hbm, v_hbm, mid_ref, wide_ref, code_ref, k_ref, v_ref, offsets, kf, vf, tf, sems):
    copies = [
        pltpu.make_async_copy(source, target, sems.at[i])
        for i, (source, target) in enumerate(
            ((offs_hbm, offsets), (k_hbm, k_ref), (v_hbm, v_ref))
        )
    ]
    for copy in copies:
        copy.start()
    first_head = lax.axis_index("sub") * 4
    copies[1].wait()
    kf[...] = k_ref[:128, :].astype(F32).T
    copies[2].wait()
    vf[...] = v_ref[:128, :].astype(F32).T
    tf[...] = jnp.concatenate([k_ref[128:192, :], v_ref[128:192, :]], axis=0).astype(F32).T
    copies[0].wait()
    code_ref[0] = sum(
        offsets[row, first_head + h] << (6 * h + 2 * row) for row in range(2) for h in range(4)
    )
    lane = lanes()
    for row, stride, out in ((0, R1, mid_ref), (1, R2, wide_ref)):
        count = out.shape[0]

        def pick(ref, h):
            return ref[pl.ds(offsets[row, first_head + h], count, stride=stride), :]

        for tile, ref in ((0, kf), (1, vf)):
            joined = jnp.where(lane < HS, pick(ref, 0), jnp.where(lane < 2 * HS, pick(ref, 1), pick(ref, 2)))
            out[:, tile * 128 : (tile + 1) * 128] = joined.astype(BF16)
        joined = jnp.where(lane % 64 < 16, pick(tf, 2), pick(tf, 3))
        out[:, 256:384] = joined.astype(BF16)


def near_kernel(offs_hbm, valid, q_ref, k_ref, v_ref, acc_ref, qm_ref, qw_ref, rows_ref, qa, ka, va, q0, q1, offsets, sem):
    rows = q_ref.shape[1]
    fetch = pltpu.make_async_copy(offs_hbm, offsets, sem)
    fetch.start()
    first_head = lax.axis_index("sub") * 4
    start = lax.axis_index("seq") * rows
    line = lax.broadcasted_iota(jnp.int32, (64, 1), 0)
    ones = jnp.broadcast_to(jnp.where(line < 4, 1.0, 0.0), (64, rows))
    q0[...] = q_ref[:128, :].astype(F32).T
    q1[...] = jnp.concatenate([q_ref[128:192, :].astype(F32), ones], axis=0).T
    qa[:, :128] = q0[...].astype(BF16)
    qa[:, 128:256] = q1[...].astype(BF16)
    position = start + lax.broadcasted_iota(jnp.int32, (1, rows), 1)
    dead = jnp.where(position < valid[0], 0.0, MASKED)
    ka[:192, :] = k_ref[...]
    ka[192:256, :] = jnp.where(line < 4, dead, 0.0).astype(BF16)
    va[:192, :] = v_ref[...]
    va[192:256, :] = ones.astype(BF16)

    chunk = 512

    def step(i, carry):
        at = pl.ds(pl.multiple_of(i * chunk, chunk), chunk)
        q = qa[at, :]

        def score(h):
            qh = jnp.where(head_lanes(h), q, jnp.zeros((), BF16))
            return jnp.dot(qh, ka[...], preferred_element_type=F32)

        acc = jnp.zeros((chunk, 256), F32)
        later = score(0)
        for h in range(4):
            scores = later
            if h < 3:
                later = score(h + 1)
            peak = jnp.max(scores, axis=1, keepdims=True)
            probs = jnp.exp2((scores - peak) * LOG2_SCALE).astype(BF16)
            out = lax.dot_general(probs, va[...], (((1,), (1,)), ((), ())), preferred_element_type=F32)
            acc = jnp.where(head_lanes(h), out, acc)
            acc = jnp.where(lanes(256) == 4 * HS + 4 + h, peak * LOG2_SCALE, acc)
        acc_ref[0, at, :] = acc[:, :128]
        acc_ref[1, at, :] = acc[:, 128:]
        return carry

    lax.fori_loop(0, rows // chunk, step, 0)

    fetch.wait()
    for row, stride, out in ((0, R1, qm_ref), (1, R2, qw_ref)):
        count = rows // stride
        for h in range(4):
            for tile, ref in ((0, q0), (1, q1)):
                picked = ref[pl.ds(offsets[row, first_head + h], count, stride=stride), :]
                picked = jnp.where(head_tile(h, tile), picked, 0.0)
                out[h * count : (h + 1) * count, tile * 128 : (tile + 1) * 128] = picked.astype(BF16)

    lane = lanes()
    one, two = normalised(acc_ref[0], acc_ref[1])
    line = lax.broadcasted_iota(jnp.int32, (rows, 1), 0)
    gone0, gone1 = False, False
    for row, stride in ((0, R1), (1, R2)):
        by0, by1 = head_vectors([offsets[row, first_head + h] for h in range(4)])
        gone0 = gone0 | ((line & (stride - 1)) == by0)
        gone1 = gone1 | ((line & (stride - 1)) == by1)
    head, tail = packed(jnp.where(gone0, 0.0, one), jnp.where(gone1, 0.0, two))
    rows_ref[: head.shape[0]] = head
    rows_ref[head.shape[0] :] = tail


def head_vectors(values):
    lane = lanes()
    first = jnp.where(lane < HS, values[0], jnp.where(lane < 2 * HS, values[1], values[2]))
    return first, jnp.where(lane < 16, values[2], values[3])


def open_piece(piece, first, stride, code, row, valid, ka, va, at):
    count = piece.shape[0]
    lane = lanes()
    shift = jnp.zeros((1, 128), jnp.int32)
    for h in range(4):
        shift = jnp.where(lane == 64 + h, offset_of(code, row, h), shift)
    position = first + stride * lax.broadcasted_iota(jnp.int32, (count, 128), 0) + shift
    mass = (lane >= 64) & (lane < 68)
    tail = piece[:, 256:384].astype(F32)
    dead = jnp.where(mass & (position >= valid[0]), MASKED, 0.0)
    ka[at, :128] = piece[:, :128]
    ka[at, 128:256] = jnp.where(lane < 64, tail, dead).astype(BF16)
    va[at, :128] = piece[:, 128:256]
    va[at, 128:256] = jnp.where(
        lane < 64, pltpu.roll(tail, 64, 1), jnp.where(mass, 1.0, 0.0)
    ).astype(BF16)


def merge(old, new, peak, h):
    before = old[1][:, 68 + h : 69 + h]
    top = jnp.maximum(before, peak)
    keep = jnp.exp2(before - top)
    add = jnp.exp2(peak - top)
    first = jnp.where(head_tile_all(h, 0), keep * old[0] + add * new[0], old[0]) if h < 3 else old[0]
    second = jnp.where(head_tile(h, 1), keep * old[1] + add * new[1], old[1])
    second = jnp.where(lanes() == 68 + h, top, second)
    return first, second


def normalised(first, second):
    lane = lanes()
    inv = [1.0 / second[:, 64 + h : 65 + h] for h in range(4)]
    one = first * jnp.where(lane < HS, inv[0], jnp.where(lane < 2 * HS, inv[1], inv[2]))
    two = second * jnp.where(lane < 16, inv[2], inv[3])
    return one, two


def packed(one, two):
    half = two.shape[0] // 2
    tail = jnp.where(lanes() < 64, two[:half], pltpu.roll(two[half:], 64, 1))
    return one.astype(BF16), tail.astype(BF16)


def middle_kernel(tok_rows, code, valid, acc_ref, qm_ref, own_ref, far_ref, swap_ref,
                  out_ref, accw_ref, ka, va, a0, a1):
    seq = lax.axis_index("seq")
    count = own_ref.shape[0]
    sources = (seq, seq ^ 2, seq ^ 1, seq ^ 3)
    pieces = (own_ref[...], far_ref[...], swap_ref[:count], swap_ref[count:])
    for i, (source, piece) in enumerate(zip(sources, pieces)):
        open_piece(piece, source * tok_rows, R1, code, 0, valid, ka, va, slice(i * count, (i + 1) * count))
    a0[...] = acc_ref[0]
    a1[...] = acc_ref[1]
    both0 = jnp.zeros((count, 128), F32)
    both1 = jnp.zeros((count, 128), F32)
    for h in range(4):
        peak, out = attend(qm_ref[h * count : (h + 1) * count], ka[...], va[...])
        at = pl.ds(offset_of(code, 0, h), count, stride=R1)
        first, second = merge((a0[at, :], a1[at, :]), (out[:, :128], out[:, 128:]), peak, h)
        both0 = jnp.where(head_tile_all(h, 0), first, both0)
        both1 = jnp.where(head_tile_all(h, 1), second, both1)
        if h < 3:
            a0[at, :] = first
        a1[at, :] = second
    wide = accw_ref.shape[1]
    first = jnp.zeros((wide, 128), F32)
    second = jnp.zeros((wide, 128), F32)
    for h in range(4):
        at = pl.ds(offset_of(code, 1, h), wide, stride=R2)
        first = jnp.where(head_tile_all(h, 0), a0[at, :], first)
        second = jnp.where(head_tile_all(h, 1), a1[at, :], second)
    accw_ref[0] = first
    accw_ref[1] = second
    one, two = normalised(both0, both1)
    line = R1 * lax.broadcasted_iota(jnp.int32, (count, 1), 0)
    mid0, mid1 = head_vectors([offset_of(code, 0, h) for h in range(4)])
    far0, far1 = head_vectors([offset_of(code, 1, h) for h in range(4)])
    gone0 = ((line + mid0) & (R2 - 1)) == far0
    gone1 = ((line + mid1) & (R2 - 1)) == far1
    head, tail = packed(jnp.where(gone0, 0.0, one), jnp.where(gone1, 0.0, two))
    out_ref[: head.shape[0]] = head
    out_ref[head.shape[0] :] = tail


def gathered_from(n_chips, side, group):
    chip = lax.axis_index("seq") // 2
    ahead = 2 * side - 1
    four, eight = n_chips // 4, n_chips // 2
    pieces = []
    for step in ((0,), (-1, 1))[group]:
        pieces += [(step, side), (step + four * ahead, side), (step + four * ahead, 1 - side), (step + eight, side)]
    if group == 0:
        for step in (2 * ahead, (2 + four) * ahead):
            pieces += [(step, side), (step, 1 - side)]
    return [(lax.rem(chip + step + n_chips, n_chips), core) for step, core in pieces]


def wide_kernel(tok_rows, n_chips, plan, last, code, valid, qw_ref, accw_ref, *refs):
    keys, (out_ref, ka, va) = refs[: len(plan)], refs[len(plan) :]
    core = lax.rem(lax.axis_index("seq"), 2)
    count = qw_ref.shape[0] // 4
    base = 0
    for (group, swapped), ref in zip(plan, keys):
        for i, (chip, core_of) in enumerate(gathered_from(n_chips, 1 - core if swapped else core, group)):
            at = slice(base, base + count)
            first = (chip * 2 + core_of) * tok_rows
            open_piece(ref[i * count : (i + 1) * count], first, R2, code, 1, valid, ka, va, at)
            base += count
    peak, out = attend(qw_ref[...], ka[...], va[...])
    first, second = accw_ref[0], accw_ref[1]
    for h in range(4):
        rows = slice(h * count, (h + 1) * count)
        first, second = merge((first, second), (out[rows, :128], out[rows, 128:]), peak[rows], h)
    if not last:
        out_ref[0] = first
        out_ref[1] = second
        return
    head, tail = packed(*normalised(first, second))
    out_ref[:count] = head
    out_ref[count:] = tail


X_FROM = (0, -1, 1, 2)


def x_sources():
    sub, subs = lax.axis_index("sub"), lax.axis_size("sub")
    return [lax.rem(sub + step + subs, subs) for step in X_FROM]


def weights_kernel(w_ref, wp):
    cols = w_ref.shape[1]
    wp[...] = jnp.zeros(wp.shape, BF16)
    for i, source in enumerate(x_sources()):
        at = pl.ds(pl.multiple_of(source * cols, cols), cols)
        for part in (0, 1):
            for low, high in ((0, 128), (128, cols)):
                piece = w_ref[at, low:high]
                wp[part, i * 256 : i * 256 + 128, low:high] = piece[:128]
                tail = i * 256 + 128 + part * 64
                wp[part, tail : tail + 64, low:high] = piece[128:]


def add_rows(refs, wp, offsets, row, stride, f0, f1):
    count = f0.shape[0] // stride
    sources = x_sources()
    for i, ref in enumerate(refs):
        tail = ref[count:].astype(F32)
        second = jnp.concatenate([tail, pltpu.roll(tail, 64, 1)], axis=0)
        both = jnp.concatenate([ref[:count].astype(F32), second], axis=1)
        stacked = jnp.concatenate(
            [jnp.where(head_lanes(h) & (lanes(256) < 4 * HS), both, 0.0) for h in range(4)], axis=0
        )
        part = jnp.dot(stacked.astype(BF16), wp[0, i * 256 : (i + 1) * 256], preferred_element_type=F32)
        for h in range(4):
            at = pl.ds(offsets[row, sources[i] * 4 + h], count, stride=stride)
            rows_h = slice(h * count, (h + 1) * count)
            f0[at, :] = f0[at, :] + part[rows_h, :128]
            f1[at, :] = f1[at, :] + part[rows_h, 128:]


def base_kernel(offs_hbm, wp, a0_ref, a1_ref, a2_ref, a3_ref, m0_ref, m1_ref, m2_ref, m3_ref,
                out_ref, f0, f1, offsets, sem):
    fetch = pltpu.make_async_copy(offs_hbm, offsets, sem)
    fetch.start()
    rows = f0.shape[0]
    half, chunk = rows // 2, 256
    for part in (0, 1):
        for start in range(0, half, chunk):
            at = slice(part * half + start, part * half + start + chunk)
            tail = slice(rows + start, rows + start + chunk)
            x = jnp.concatenate(
                [piece for ref in (a0_ref, a1_ref, a2_ref, a3_ref) for piece in (ref[at], ref[tail])], axis=1
            )
            total = jnp.dot(x, wp[part], preferred_element_type=F32)
            f0[at, :] = total[:, :128]
            f1[at, :] = total[:, 128:]
    fetch.wait()
    add_rows((m0_ref, m1_ref, m2_ref, m3_ref), wp, offsets, 0, R1, f0, f1)
    out_ref[0] = f0[...]
    out_ref[1] = f1[...]


def final_kernel(offs_hbm, valid, wp, base_ref, b0_ref, b1_ref, b2_ref, b3_ref, out_ref, f0, f1, offsets, sem):
    cols, rows = out_ref.shape
    fetch = pltpu.make_async_copy(offs_hbm, offsets, sem)
    fetch.start()
    f0[...] = base_ref[0]
    f1[...] = base_ref[1]
    fetch.wait()
    add_rows((b0_ref, b1_ref, b2_ref, b3_ref), wp, offsets, 1, R2, f0, f1)
    position = lax.axis_index("seq") * rows + lax.broadcasted_iota(jnp.int32, (1, rows), 1)
    keep = position < valid[0]
    out_ref[:128, :] = jnp.where(keep, f0[...].T, 0.0).astype(BF16)
    out_ref[128:, :] = jnp.where(keep, f1[...].T[: cols - 128], 0.0).astype(BF16)


HBM = pl.BlockSpec(memory_space=pltpu.HBM)


def call(body, ins, outs, scratch, flops, limit=20):
    return pl.pallas_call(
        body,
        out_shape=[jax.ShapeDtypeStruct(s, d) for s, d in outs],
        in_specs=[{"s": SMEM, "v": VMEM, "a": HBM}[kind] for kind in ins],
        out_specs=[SMEM if d == jnp.int32 else VMEM for _, d in outs],
        scratch_shapes=[s if not isinstance(s, tuple) else pltpu.VMEM(*s) for s in scratch],
        cost_estimate=pl.CostEstimate(flops=int(flops), bytes_accessed=2 << 20, transcendentals=0),
        compiler_params=pltpu.CompilerParams(vmem_limit_bytes=limit << 20),
    )


def local(q_heads, k_heads, v_heads, w_out, offsets, valid):
    rows, cols = q_heads.shape
    sub = lax.axis_index("sub")
    n_seq = lax.axis_size("seq")
    n_sub = lax.axis_size("sub")
    n_chips = n_seq // 2
    mid, wide = rows // R1, rows // R2
    w_cols = lax.dynamic_slice_in_dim(w_out, sub * cols, cols, 1)

    def along_z(value, up, down):
        pairs = [(2 * z + c, 2 * ((z + (up, down)[c]) % n_chips) + c) for z in range(n_chips) for c in (0, 1)]
        return lax.ppermute(value, "seq", pairs)

    def flipped(value, mask):
        return lax.ppermute(value, "seq", [(i, i ^ mask) for i in range(n_seq)])

    def along_x(value, step):
        return lax.ppermute(value, "sub", [(i, (i + step) % n_sub) for i in range(n_sub)])

    smem_offsets = pltpu.SMEM(offsets.shape, jnp.int32)
    q_t, k_t, v_t = q_heads.T, k_heads.T, v_heads.T
    kv_mid, kv_wide, own_code = call(
        prep_kernel, "aaa",
        [((mid, 384), BF16), ((wide, 384), BF16), ((1,), jnp.int32)],
        [((cols, rows), BF16)] * 2 + [smem_offsets] + [((rows, 128), F32)] * 3 + [pltpu.SemaphoreType.DMA((3,))],
        2e8, 60,
    )(offsets, k_t, v_t)

    code = own_code | (sub << 24)
    near_q, w_cols, code = lax.optimization_barrier((q_t, w_cols, code))
    four = n_chips // 4
    kv_both = flipped(kv_wide, 1)
    far_mid = flipped(kv_mid, 2)
    own_pair = jnp.concatenate([kv_wide, kv_both], axis=0)
    far4 = along_z(own_pair, four, -four)
    packed_rows = rows + rows // 2
    acc, q_mid, q_wide, attn = call(
        near_kernel, "asvvv",
        [((2, rows, 128), F32), ((4 * mid, 256), BF16), ((4 * wide, 256), BF16), ((packed_rows, 128), BF16)],
        [((rows, 256), BF16), ((256, rows), BF16), ((256, rows), BF16)] + [((rows, 128), F32)] * 2
        + [smem_offsets, pltpu.SemaphoreType.DMA],
        4e9, 28,
    )(offsets, valid, near_q, k_t, v_t)
    far_mid, acc = lax.optimization_barrier((far_mid, acc))
    attns = [along_x(attn, s) for s in (1, n_sub - 1, 2)]

    swap_mid = flipped(jnp.concatenate([kv_mid, far_mid], axis=0), 1)
    far8 = along_z(far4[:wide], four, -four)
    mine = jnp.concatenate([kv_wide, far4, far8], axis=0)
    around2 = along_z(jnp.concatenate([own_pair, far4], axis=0), 2, -2)
    around_up = along_z(mine, 1, 1)
    around_down = along_z(mine, -1, -1)
    attn_mid, acc_wide = call(
        functools.partial(middle_kernel, rows), "ssvvvvv",
        [((mid + mid // 2, 128), BF16), ((2, wide, 128), F32)],
        [((4 * mid, 256), BF16)] * 2 + [((rows, 128), F32)] * 2,
        1e9,
    )(code, valid, acc, q_mid, kv_mid, far_mid, swap_mid)
    mids = [along_x(attn_mid, s) for s in (1, n_sub - 1, 2)]

    def wide_part(plan, acc_now, keys, last=False):
        n_keys = sum(k.shape[0] for k in keys)
        (result,) = call(
            functools.partial(wide_kernel, rows, n_chips, plan, last), "ssvv" + "v" * len(keys),
            [((wide + wide // 2, 128), BF16) if last else ((2, wide, 128), F32)],
            [((n_keys, 256), BF16)] * 2, 5e8,
        )(code, valid, q_wide, acc_now, *keys)
        return result

    early = jnp.concatenate([mine, around2], axis=0)
    early_other = flipped(early, 1)
    late = jnp.concatenate([around_up, around_down], axis=0)
    late_other = flipped(late, 1)
    acc_wide = wide_part(((0, False), (0, True)), acc_wide, (early, early_other))
    acc_wide = wide_part(((1, False),), acc_wide, (late,))
    attn_wide = wide_part(((1, True),), acc_wide, (late_other,), last=True)
    (w_blocks,) = call(weights_kernel, "v", [((2, 4 * 256, 256), BF16)], [], 1e7)(w_cols)
    wides = [along_x(attn_wide, s) for s in (1, n_sub - 1, 2)]
    pair_of_tiles = [((rows, 128), F32)] * 2 + [smem_offsets, pltpu.SemaphoreType.DMA]
    (base,) = call(
        base_kernel, "av" + "v" * 8, [((2, rows, 128), F32)], pair_of_tiles, 1e9,
    )(offsets, w_blocks, attn, *attns, attn_mid, *mids)
    (out,) = call(
        final_kernel, "asv" + "v" * 5, [((cols, rows), BF16)], pair_of_tiles, 5e8,
    )(offsets, valid, w_blocks, base, attn_wide, *wides)
    return out.T


def solution(mesh):
    placed = (
        P(("slides", "seq"), "sub"),
        P(("slides", "seq"), "sub"),
        P(("slides", "seq"), "sub"),
        P(),
        P(),
        P("slides"),
    )


    return jax.shard_map(local, mesh=mesh, in_specs=placed, out_specs=P(("slides", "seq"), "sub"), check_vma=False)
```

```python
import functools
import math

import jax
import jax.numpy as jnp
from jax import lax
from jax.experimental import pallas as pl
from jax.experimental.pallas import tpu as pltpu
from jax.sharding import PartitionSpec as P


HS = 48
R1 = 4
R2 = 16
LOG2_SCALE = HS ** (-0.5) * math.log2(math.e)
MASKED = -1e6

F32 = jnp.float32
BF16 = jnp.bfloat16


VMEM = pl.BlockSpec(memory_space=pltpu.VMEM)
SMEM = pl.BlockSpec(memory_space=pltpu.SMEM)


def lanes(width=128):
    return lax.broadcasted_iota(jnp.int32, (1, width), 1)


def head_lanes(h):
    lane = lanes(256)
    return ((lane >= h * HS) & (lane < (h + 1) * HS)) | (lane == 4 * HS + h)


def head_tile(h, tile):
    return head_lanes(h)[:, tile * 128 : (tile + 1) * 128]


def head_tile_all(h, tile):
    lane = lanes()
    if tile == 0:
        return (lane >= h * HS) & (lane < (h + 1) * HS)
    low = h * HS - 128
    return ((lane >= low) & (lane < low + HS) & (lane < 64)) | (lane == 64 + h) | (lane == 68 + h)


def offset_of(code, row, h):
    return (code[0] >> (6 * h + 2 * row)) & (R1 - 1, R2 - 1)[row]


def attend(q, k, v, k_dims=(1,), v_dims=(0,)):
    scores = lax.dot_general(q, k, (((1,), k_dims), ((), ())), preferred_element_type=F32)
    peak = jnp.max(scores, axis=1, keepdims=True)
    probs = jnp.exp2((scores - peak) * LOG2_SCALE).astype(BF16)
    out = lax.dot_general(probs, v, (((1,), v_dims), ((), ())), preferred_element_type=F32)
    return peak * LOG2_SCALE, out


def prep_kernel(offs_hbm, k_hbm, v_hbm, mid_ref, wide_ref, code_ref, k_ref, v_ref, offsets, kf, vf, tf, sems):
    copies = [
        pltpu.make_async_copy(source, target, sems.at[i])
        for i, (source, target) in enumerate(
            ((offs_hbm, offsets), (k_hbm, k_ref), (v_hbm, v_ref))
        )
    ]
    for copy in copies:
        copy.start()
    first_head = lax.axis_index("sub") * 4
    copies[1].wait()
    kf[...] = k_ref[:128, :].astype(F32).T
    copies[2].wait()
    vf[...] = v_ref[:128, :].astype(F32).T
    tf[...] = jnp.concatenate([k_ref[128:192, :], v_ref[128:192, :]], axis=0).astype(F32).T
    copies[0].wait()
    code_ref[0] = sum(
        offsets[row, first_head + h] << (6 * h + 2 * row) for row in range(2) for h in range(4)
    )
    lane = lanes()
    for row, stride, out in ((0, R1, mid_ref), (1, R2, wide_ref)):
        count = out.shape[0]

        def pick(ref, h):
            return ref[pl.ds(offsets[row, first_head + h], count, stride=stride), :]

        for tile, ref in ((0, kf), (1, vf)):
            joined = jnp.where(lane < HS, pick(ref, 0), jnp.where(lane < 2 * HS, pick(ref, 1), pick(ref, 2)))
            out[:, tile * 128 : (tile + 1) * 128] = joined.astype(BF16)
        joined = jnp.where(lane % 64 < 16, pick(tf, 2), pick(tf, 3))
        out[:, 256:384] = joined.astype(BF16)


def near_kernel(offs_hbm, valid, q_ref, k_ref, v_ref, acc_ref, qm_ref, qw_ref, qa, ka, va, q0, q1, offsets, sem):
    rows = q_ref.shape[1]
    fetch = pltpu.make_async_copy(offs_hbm, offsets, sem)
    fetch.start()
    first_head = lax.axis_index("sub") * 4
    start = lax.axis_index("seq") * rows
    line = lax.broadcasted_iota(jnp.int32, (64, 1), 0)
    ones = jnp.broadcast_to(jnp.where(line < 4, 1.0, 0.0), (64, rows))
    q0[...] = q_ref[:128, :].astype(F32).T
    q1[...] = jnp.concatenate([q_ref[128:192, :].astype(F32), ones], axis=0).T
    qa[:, :128] = q0[...].astype(BF16)
    qa[:, 128:256] = q1[...].astype(BF16)
    position = start + lax.broadcasted_iota(jnp.int32, (1, rows), 1)
    dead = jnp.where(position < valid[0], 0.0, MASKED)
    ka[:192, :] = k_ref[...]
    ka[192:256, :] = jnp.where(line < 4, dead, 0.0).astype(BF16)
    va[:192, :] = v_ref[...]
    va[192:256, :] = ones.astype(BF16)

    chunk = 512

    def step(i, carry):
        at = pl.ds(pl.multiple_of(i * chunk, chunk), chunk)
        q = qa[at, :]

        def score(h):
            qh = jnp.where(head_lanes(h), q, jnp.zeros((), BF16))
            return jnp.dot(qh, ka[...], preferred_element_type=F32)

        acc = jnp.zeros((chunk, 256), F32)
        later = score(0)
        for h in range(4):
            scores = later
            if h < 3:
                later = score(h + 1)
            peak = jnp.max(scores, axis=1, keepdims=True)
            probs = jnp.exp2((scores - peak) * LOG2_SCALE).astype(BF16)
            out = lax.dot_general(probs, va[...], (((1,), (1,)), ((), ())), preferred_element_type=F32)
            acc = jnp.where(head_lanes(h), out, acc)
            acc = jnp.where(lanes(256) == 4 * HS + 4 + h, peak * LOG2_SCALE, acc)
        acc_ref[0, at, :] = acc[:, :128]
        acc_ref[1, at, :] = acc[:, 128:]
        return carry

    lax.fori_loop(0, rows // chunk, step, 0)

    fetch.wait()
    for row, stride, out in ((0, R1, qm_ref), (1, R2, qw_ref)):
        count = rows // stride
        for h in range(4):
            for tile, ref in ((0, q0), (1, q1)):
                picked = ref[pl.ds(offsets[row, first_head + h], count, stride=stride), :]
                picked = jnp.where(head_tile(h, tile), picked, 0.0)
                out[h * count : (h + 1) * count, tile * 128 : (tile + 1) * 128] = picked.astype(BF16)


def open_piece(piece, first, stride, code, row, valid, ka, va, at):
    count = piece.shape[0]
    lane = lanes()
    shift = jnp.zeros((1, 128), jnp.int32)
    for h in range(4):
        shift = jnp.where(lane == 64 + h, offset_of(code, row, h), shift)
    position = first + stride * lax.broadcasted_iota(jnp.int32, (count, 128), 0) + shift
    mass = (lane >= 64) & (lane < 68)
    tail = piece[:, 256:384].astype(F32)
    dead = jnp.where(mass & (position >= valid[0]), MASKED, 0.0)
    ka[at, :128] = piece[:, :128]
    ka[at, 128:256] = jnp.where(lane < 64, tail, dead).astype(BF16)
    va[at, :128] = piece[:, 128:256]
    va[at, 128:256] = jnp.where(
        lane < 64, pltpu.roll(tail, 64, 1), jnp.where(mass, 1.0, 0.0)
    ).astype(BF16)


def merge(old, new, peak, h):
    before = old[1][:, 68 + h : 69 + h]
    top = jnp.maximum(before, peak)
    keep = jnp.exp2(before - top)
    add = jnp.exp2(peak - top)
    first = jnp.where(head_tile_all(h, 0), keep * old[0] + add * new[0], old[0]) if h < 3 else old[0]
    second = jnp.where(head_tile(h, 1), keep * old[1] + add * new[1], old[1])
    second = jnp.where(lanes() == 68 + h, top, second)
    return first, second


def normalised(first, second):
    lane = lanes()
    inv = [1.0 / second[:, 64 + h : 65 + h] for h in range(4)]
    one = first * jnp.where(lane < HS, inv[0], jnp.where(lane < 2 * HS, inv[1], inv[2]))
    two = second * jnp.where(lane < 16, inv[2], inv[3])
    return one, two


def packed(one, two):
    half = two.shape[0] // 2
    tail = jnp.where(lanes() < 64, two[:half], pltpu.roll(two[half:], 64, 1))
    return one.astype(BF16), tail.astype(BF16)


def middle_kernel(tok_rows, code, valid, acc_ref, qm_ref, own_ref, far_ref, swap_ref,
                  out_ref, accw_ref, ka, va, a0, a1):
    seq = lax.axis_index("seq")
    count = own_ref.shape[0]
    sources = (seq, seq ^ 2, seq ^ 1, seq ^ 3)
    pieces = (own_ref[...], far_ref[...], swap_ref[:count], swap_ref[count:])
    for i, (source, piece) in enumerate(zip(sources, pieces)):
        open_piece(piece, source * tok_rows, R1, code, 0, valid, ka, va, slice(i * count, (i + 1) * count))
    a0[...] = acc_ref[0]
    a1[...] = acc_ref[1]
    for h in range(4):
        peak, out = attend(qm_ref[h * count : (h + 1) * count], ka[...], va[...])
        at = pl.ds(offset_of(code, 0, h), count, stride=R1)
        first, second = merge((a0[at, :], a1[at, :]), (out[:, :128], out[:, 128:]), peak, h)
        if h < 3:
            a0[at, :] = first
        a1[at, :] = second
    wide = accw_ref.shape[1]
    first = jnp.zeros((wide, 128), F32)
    second = jnp.zeros((wide, 128), F32)
    for h in range(4):
        at = pl.ds(offset_of(code, 1, h), wide, stride=R2)
        here0, here1 = a0[at, :], a1[at, :]
        first = jnp.where(head_tile_all(h, 0), here0, first)
        second = jnp.where(head_tile_all(h, 1), here1, second)
        if h < 3:
            a0[at, :] = jnp.where(head_tile_all(h, 0), 0.0, here0)
        if h > 1:
            a1[at, :] = jnp.where(head_tile_all(h, 1) & (lanes() < 64), 0.0, here1)
    accw_ref[0] = first
    accw_ref[1] = second
    one, two = normalised(a0[...], a1[...])
    head, tail = packed(one, two)
    out_ref[: head.shape[0]] = head
    out_ref[head.shape[0] :] = tail


def gathered_from(n_chips, side, group):
    chip = lax.axis_index("seq") // 2
    ahead = 2 * side - 1
    four, eight = n_chips // 4, n_chips // 2
    pieces = []
    for step in ((0,), (-1, 1))[group]:
        pieces += [(step, side), (step + four * ahead, side), (step + four * ahead, 1 - side), (step + eight, side)]
    if group == 0:
        for step in (2 * ahead, (2 + four) * ahead):
            pieces += [(step, side), (step, 1 - side)]
    return [(lax.rem(chip + step + n_chips, n_chips), core) for step, core in pieces]


def wide_kernel(tok_rows, n_chips, plan, last, code, valid, qw_ref, accw_ref, *refs):
    keys, (out_ref, ka, va) = refs[: len(plan)], refs[len(plan) :]
    core = lax.rem(lax.axis_index("seq"), 2)
    count = qw_ref.shape[0] // 4
    base = 0
    for (group, swapped), ref in zip(plan, keys):
        for i, (chip, core_of) in enumerate(gathered_from(n_chips, 1 - core if swapped else core, group)):
            at = slice(base, base + count)
            first = (chip * 2 + core_of) * tok_rows
            open_piece(ref[i * count : (i + 1) * count], first, R2, code, 1, valid, ka, va, at)
            base += count
    peak, out = attend(qw_ref[...], ka[...], va[...])
    first, second = accw_ref[0], accw_ref[1]
    for h in range(4):
        rows = slice(h * count, (h + 1) * count)
        first, second = merge((first, second), (out[rows, :128], out[rows, 128:]), peak[rows], h)
    if not last:
        out_ref[0] = first
        out_ref[1] = second
        return
    head, tail = packed(*normalised(first, second))
    out_ref[:count] = head
    out_ref[count:] = tail


X_FROM = (0, -1, 1, 2)


def x_sources():
    sub, subs = lax.axis_index("sub"), lax.axis_size("sub")
    return [lax.rem(sub + step + subs, subs) for step in X_FROM]


def weights_kernel(w_ref, wp):
    cols = w_ref.shape[1]
    wp[...] = jnp.zeros(wp.shape, BF16)
    for i, source in enumerate(x_sources()):
        at = pl.ds(pl.multiple_of(source * cols, cols), cols)
        for part in (0, 1):
            for low, high in ((0, 128), (128, cols)):
                piece = w_ref[at, low:high]
                wp[part, i * 256 : i * 256 + 128, low:high] = piece[:128]
                tail = i * 256 + 128 + part * 64
                wp[part, tail : tail + 64, low:high] = piece[128:]


def final_kernel(offs_hbm, valid, wp, a0_ref, a1_ref, a2_ref, a3_ref, b0_ref, b1_ref, b2_ref, b3_ref,
                 out_ref, f0, f1, offsets, sem):
    cols, rows = out_ref.shape
    fetch = pltpu.make_async_copy(offs_hbm, offsets, sem)
    fetch.start()
    half, count, chunk = rows // 2, rows // R2, 256
    sources = x_sources()
    for part in (0, 1):
        for start in range(0, half, chunk):
            at = slice(part * half + start, part * half + start + chunk)
            tail = slice(rows + start, rows + start + chunk)
            x = jnp.concatenate(
                [piece for ref in (a0_ref, a1_ref, a2_ref, a3_ref) for piece in (ref[at], ref[tail])], axis=1
            )
            total = jnp.dot(x, wp[part], preferred_element_type=F32)
            f0[at, :] = total[:, :128]
            f1[at, :] = total[:, 128:]
    fetch.wait()
    for i, ref in enumerate((b0_ref, b1_ref, b2_ref, b3_ref)):
        tail = ref[count:].astype(F32)
        second = jnp.concatenate([tail, pltpu.roll(tail, 64, 1)], axis=0)
        both = jnp.concatenate([ref[:count].astype(F32), second], axis=1)
        stacked = jnp.concatenate(
            [jnp.where(head_lanes(h) & (lanes(256) < 4 * HS), both, 0.0) for h in range(4)], axis=0
        )
        part = jnp.dot(stacked.astype(BF16), wp[0, i * 256 : (i + 1) * 256], preferred_element_type=F32)
        for h in range(4):
            at = pl.ds(offsets[1, sources[i] * 4 + h], count, stride=R2)
            rows_h = slice(h * count, (h + 1) * count)
            f0[at, :] = f0[at, :] + part[rows_h, :128]
            f1[at, :] = f1[at, :] + part[rows_h, 128:]
    position = lax.axis_index("seq") * rows + lax.broadcasted_iota(jnp.int32, (1, rows), 1)
    keep = position < valid[0]
    out_ref[:128, :] = jnp.where(keep, f0[...].T, 0.0).astype(BF16)
    out_ref[128:, :] = jnp.where(keep, f1[...].T[: cols - 128], 0.0).astype(BF16)


HBM = pl.BlockSpec(memory_space=pltpu.HBM)


def call(body, ins, outs, scratch, flops, limit=20):
    return pl.pallas_call(
        body,
        out_shape=[jax.ShapeDtypeStruct(s, d) for s, d in outs],
        in_specs=[{"s": SMEM, "v": VMEM, "a": HBM}[kind] for kind in ins],
        out_specs=[SMEM if d == jnp.int32 else VMEM for _, d in outs],
        scratch_shapes=[s if not isinstance(s, tuple) else pltpu.VMEM(*s) for s in scratch],
        cost_estimate=pl.CostEstimate(flops=int(flops), bytes_accessed=2 << 20, transcendentals=0),
        compiler_params=pltpu.CompilerParams(vmem_limit_bytes=limit << 20),
    )


def local(q_heads, k_heads, v_heads, w_out, offsets, valid):
    rows, cols = q_heads.shape
    sub = lax.axis_index("sub")
    n_seq = lax.axis_size("seq")
    n_sub = lax.axis_size("sub")
    n_chips = n_seq // 2
    mid, wide = rows // R1, rows // R2
    w_cols = lax.dynamic_slice_in_dim(w_out, sub * cols, cols, 1)

    def along_z(value, up, down):
        pairs = [(2 * z + c, 2 * ((z + (up, down)[c]) % n_chips) + c) for z in range(n_chips) for c in (0, 1)]
        return lax.ppermute(value, "seq", pairs)

    def flipped(value, mask):
        return lax.ppermute(value, "seq", [(i, i ^ mask) for i in range(n_seq)])

    def along_x(value, step):
        return lax.ppermute(value, "sub", [(i, (i + step) % n_sub) for i in range(n_sub)])

    smem_offsets = pltpu.SMEM(offsets.shape, jnp.int32)
    q_t, k_t, v_t = q_heads.T, k_heads.T, v_heads.T
    kv_mid, kv_wide, own_code = call(
        prep_kernel, "aaa",
        [((mid, 384), BF16), ((wide, 384), BF16), ((1,), jnp.int32)],
        [((cols, rows), BF16)] * 2 + [smem_offsets] + [((rows, 128), F32)] * 3 + [pltpu.SemaphoreType.DMA((3,))],
        2e8, 60,
    )(offsets, k_t, v_t)

    code = own_code | (sub << 24)
    near_q, w_cols, code = lax.optimization_barrier((q_t, w_cols, code))
    four = n_chips // 4
    kv_both = flipped(kv_wide, 1)
    far_mid = flipped(kv_mid, 2)
    own_pair = jnp.concatenate([kv_wide, kv_both], axis=0)
    far4 = along_z(own_pair, four, -four)
    acc, q_mid, q_wide = call(
        near_kernel, "asvvv",
        [((2, rows, 128), F32), ((4 * mid, 256), BF16), ((4 * wide, 256), BF16)],
        [((rows, 256), BF16), ((256, rows), BF16), ((256, rows), BF16)] + [((rows, 128), F32)] * 2
        + [smem_offsets, pltpu.SemaphoreType.DMA],
        4e9, 28,
    )(offsets, valid, near_q, k_t, v_t)
    far_mid, acc = lax.optimization_barrier((far_mid, acc))

    swap_mid = flipped(jnp.concatenate([kv_mid, far_mid], axis=0), 1)
    far8 = along_z(far4[:wide], four, -four)
    mine = jnp.concatenate([kv_wide, far4, far8], axis=0)
    around2 = along_z(jnp.concatenate([own_pair, far4], axis=0), 2, -2)
    around_up = along_z(mine, 1, 1)
    around_down = along_z(mine, -1, -1)
    attn, acc_wide = call(
        functools.partial(middle_kernel, rows), "ssvvvvv",
        [((rows + rows // 2, 128), BF16), ((2, wide, 128), F32)],
        [((4 * mid, 256), BF16)] * 2 + [((rows, 128), F32)] * 2,
        1e9,
    )(code, valid, acc, q_mid, kv_mid, far_mid, swap_mid)
    attns = [along_x(attn, s) for s in (1, n_sub - 1, 2)]

    def wide_part(plan, acc_now, keys, last=False):
        n_keys = sum(k.shape[0] for k in keys)
        (result,) = call(
            functools.partial(wide_kernel, rows, n_chips, plan, last), "ssvv" + "v" * len(keys),
            [((wide + wide // 2, 128), BF16) if last else ((2, wide, 128), F32)],
            [((n_keys, 256), BF16)] * 2, 5e8,
        )(code, valid, q_wide, acc_now, *keys)
        return result

    early = jnp.concatenate([mine, around2], axis=0)
    early_other = flipped(early, 1)
    late = jnp.concatenate([around_up, around_down], axis=0)
    late_other = flipped(late, 1)
    acc_wide = wide_part(((0, False), (0, True)), acc_wide, (early, early_other))
    acc_wide = wide_part(((1, False),), acc_wide, (late,))
    attn_wide = wide_part(((1, True),), acc_wide, (late_other,), last=True)
    (w_blocks,) = call(weights_kernel, "v", [((2, 4 * 256, 256), BF16)], [], 1e7)(w_cols)
    wides = [along_x(attn_wide, s) for s in (1, n_sub - 1, 2)]
    (out,) = call(
        final_kernel, "asv" + "v" * 8, [((cols, rows), BF16)],
        [((rows, 128), F32)] * 2
        + [smem_offsets, pltpu.SemaphoreType.DMA], 1e9,
    )(offsets, valid, w_blocks, attn, *attns, attn_wide, *wides)
    return out.T


def solution(mesh):
    placed = (
        P(("slides", "seq"), "sub"),
        P(("slides", "seq"), "sub"),
        P(("slides", "seq"), "sub"),
        P(),
        P(),
        P("slides"),
    )


    return jax.shard_map(local, mesh=mesh, in_specs=placed, out_specs=P(("slides", "seq"), "sub"), check_vma=False)
```
